128 devices in a mesh: tm: 64 (over y, x, z), batch: 2 (over core).
Axes of the slice: x: 4, y: 4, z: 4, core: 2. Of those that a mesh axis runs over, the one named last changes fastest.
Arguments:
- state_map: float32 [2048, 256, 256], P(('batch', 'tm')), parts along dimension 0, may hold values from -0.375 to 0.375
- input_map: float32 [2048, 64, 256], P(('batch', 'tm')), parts along dimension 0, may hold values from -0.375 to 0.375
- closed_loop: float32 [2048, 256, 256], P(('batch', 'tm')), parts along dimension 0, may hold values from -1.001 to 1.001
- feedback: float32 [2048, 64, 256], P(('batch', 'tm')), parts along dimension 0, may hold values from -0.375 to 0.375
- value_matrix: float32 [2048, 256, 256], P(('batch', 'tm')), parts along dimension 0, may hold values from -0.046875 to 1.5, as said below
- gain_inverse: float32 [2048, 64, 64], P(('batch', 'tm')), parts along dimension 0, may hold values from -0.0105 to 0.2, as said below
- input_weight: float32 [128, 64], P('batch'), parts along dimension 0, may hold values from -0.36 to 6, as said below
- state_weight: float32 [2048, 256], P(('batch', 'tm')), parts along dimension 0, may hold values from 0.1 to 3
- state_linear: float32 [2048, 256], P(('batch', 'tm')), parts along dimension 0, may hold values from -0.18 to 0.18
- input_linear: float32 [2048, 64], P(('batch', 'tm')), parts along dimension 0, may hold values from -0.18 to 0.18
- offset: float32 [2048, 256], P(('batch', 'tm')), parts along dimension 0, may hold values from -0.18 to 0.18
- upper_bound: float32 [2048, 64], P(('batch', 'tm')), parts along dimension 0, may hold values from 0.1 to 0.3
- states: float32 [2048, 256], P(('batch', 'tm')), parts along dimension 0, may hold values from -0.18 to 0.18
- inputs: float32 [2048, 64], P(('batch', 'tm')), parts along dimension 0, may hold values from -0.18 to 0.18
- multipliers: float32 [2048, 256], P(('batch', 'tm')), parts along dimension 0, may hold values from -0.18 to 0.18
- bound_mult: float32 [2048, 64], P(('batch', 'tm')), parts along dimension 0, may hold values from 0 to 0.06
- active: int32 [2048, 64], P(('batch', 'tm')), parts along dimension 0, may hold values 0 or 1
Outputs:
- state_step: float32 [2048, 256], P(('batch', 'tm')), parts along dimension 0
- input_step: float32 [2048, 64], P(('batch', 'tm')), parts along dimension 0
- multiplier_step: float32 [2048, 256], P(('batch', 'tm')), parts along dimension 0
- bound_step: float32 [2048, 64], P(('batch', 'tm')), parts along dimension 0
- kkt_norms: float32 [6], P('batch'), parts along dimension 0
The draws below stay inside these ranges and needn't reach their ends.
There are 2 independent parts, one for each index of `batch`. The reference program is written for one: setup_inputs(seed, part) draws one part's arguments, and reference() takes and returns one part's arrays. A program takes and returns all parts, laid end to end along the dimension named above; each array names one. Nothing has to cross between parts.
Inputs may be any that keep to these rules, and one draw needn't show every extreme that they name: `value_matrix`: each section's matrix is symmetric. `gain_inverse`: each section's matrix is symmetric. `input_weight`: symmetric.
All inputs are finite; a program needn't handle non-finite values. No bound on the sum of `active` on one device may be relied on, other than what follows from the above.
Results may differ from the reference program's by a relative error of at most 0.0003.
Values sent between devices are 32-bit elements; how exact they have to be, the bound alone decides.
A program may use at most 128 MiB of HBM per device.

```python
import math
import jax
import jax.numpy as jnp
from jax import lax

NS = 256
NU = 64
HORIZON = 1024


def symmetric_draw(key, sections, dimension, lowest, highest, spread):
    first_key, second_key = jax.random.split(key)
    diagonal = jax.random.uniform(first_key, (sections, dimension), jnp.float32, lowest, highest)
    noise_raw = jax.random.normal(second_key, (sections, dimension, dimension), jnp.float32) * spread
    mixed = jnp.clip((noise_raw + jnp.swapaxes(noise_raw, 1, 2)) / math.sqrt(2.0), -3.0 * spread, 3.0 * spread)
    identity = jnp.eye(dimension, dtype=jnp.float32)
    return mixed * (1.0 - identity) + diagonal[:, :, None] * identity


def draw_value_matrix(key, part):
    return symmetric_draw(jax.random.fold_in(key, 11), HORIZON, NS, 0.5, 1.5, 0.25 / math.sqrt(NS))


def draw_gain_inverse(key, part):
    return symmetric_draw(jax.random.fold_in(key, 12), HORIZON, NU, 0.08, 0.2, 0.028 / math.sqrt(NU))


def draw_input_weight(key, part):
    return symmetric_draw(jax.random.fold_in(key, 13), 1, NU, 2.0, 6.0, 0.96 / math.sqrt(NU))[0]


def draw_closed_loop(key, part):
    subkeys = jax.random.split(jax.random.fold_in(key, 7), 5)
    ranking = jax.random.permutation(subkeys[0], NS)
    slow_total = NS // 2
    slow_channel = ranking < slow_total
    same_class = (slow_channel[:, None] == slow_channel[None, :]).astype(jnp.float32)
    slow_rate = jax.random.uniform(subkeys[1], (HORIZON, NS), jnp.float32, 0.3, 2.0) / HORIZON
    memory = jnp.exp(jax.random.uniform(subkeys[2], (HORIZON, NS), jnp.float32, math.log(2.0), math.log(8.0)))
    decays = jnp.where(slow_channel[None, :], jnp.exp(-slow_rate), jnp.exp(-1.0 / memory))
    noise_raw = jax.random.normal(subkeys[3], (HORIZON, NS, NS), jnp.float32) * (0.5 / math.sqrt(NS))
    cross_raw = jax.random.normal(subkeys[4], (HORIZON, NS, NS), jnp.float32) * (0.25 / math.sqrt(NS * HORIZON))
    within_part = (noise_raw - jnp.swapaxes(noise_raw, 1, 2)) * same_class
    between_part = (cross_raw - jnp.swapaxes(cross_raw, 1, 2)) * (1.0 - same_class)
    skew_part = within_part + between_part
    identity = jnp.eye(NS, dtype=jnp.float32)
    rotation = jnp.linalg.solve(identity + skew_part, identity - skew_part)
    return decays[:, :, None] * rotation


def with_ends(array, stream_key, low, top_value):
    spot = [jax.random.randint(jax.random.fold_in(stream_key, axis), (), 0, length) for axis, length in enumerate(array.shape)]
    main_axis = array.shape.index(max(array.shape))
    next_to = spot[:main_axis] + [(spot[main_axis] + 1) % array.shape[main_axis]] + spot[main_axis + 1:]
    return array.at[tuple(spot)].set(low).at[tuple(next_to)].set(top_value)


def block_scale(key, dims, shards, low, high):
    level = 1.0
    for axis_at, blocks in shards:
        draws = jax.random.uniform(jax.random.fold_in(jax.random.fold_in(key, 6), axis_at), (blocks,), jnp.float32, low / len(shards), high / len(shards))
        level = level * jnp.repeat(jnp.exp(draws), dims[axis_at] // blocks).reshape((-1,) + (1,) * (len(dims) - 1 - axis_at))
    return level


def noise(own_key, shape, scale, limit, cuts=(), kind=jnp.bfloat16):
    drawn = jax.random.normal(own_key, shape, jnp.float32) * scale
    if len(cuts) > 0:
        drawn = block_scale(own_key, shape, cuts, -0.22, 0.18) * drawn
    return jnp.clip(drawn, min=-limit, max=limit).astype(kind)


def setup_inputs(seed: int = 0, part: int = 0) -> dict:
    key_list = jax.random.split(jax.random.key(seed), 18)
    part_splits = jax.random.split(jax.random.fold_in(key_list[17], part), 18)
    state_map = noise(part_splits[0], (HORIZON, NS, NS), NS ** -0.5, 0.375, ((0, 64),), jnp.float32)
    input_map = noise(part_splits[1], (HORIZON, NU, NS), NS ** -0.5, 0.375, ((0, 64),), jnp.float32)
    closed_loop = draw_closed_loop(jax.random.fold_in(jax.random.fold_in(key_list[17], part), 71), part)
    feedback = noise(part_splits[3], (HORIZON, NU, NS), NS ** -0.5, 0.375, ((0, 64),), jnp.float32)
    value_matrix = draw_value_matrix(jax.random.fold_in(jax.random.fold_in(key_list[17], part), 71), part)
    gain_inverse = draw_gain_inverse(jax.random.fold_in(jax.random.fold_in(key_list[17], part), 71), part)
    input_weight = draw_input_weight(jax.random.fold_in(jax.random.fold_in(key_list[17], part), 71), part)
    state_weight = jnp.clip(jnp.exp(math.log(3.0) - 3.4011974 * jax.random.uniform(part_splits[7], (HORIZON, NS), jnp.float32) ** block_scale(part_splits[7], (HORIZON, NS), ((0, 64),), -0.2, 0.2)), 0.1, 3.0)
    state_linear = noise(part_splits[8], (HORIZON, NS), 0.03, 0.18, ((0, 64),), jnp.float32)
    input_linear = noise(part_splits[9], (HORIZON, NU), 0.03, 0.18, ((0, 64),), jnp.float32)
    offset = noise(part_splits[10], (HORIZON, NS), 0.03, 0.18, ((0, 64),), jnp.float32)
    upper_bound = jnp.clip(0.1 + 0.20000001043081284 * jax.random.uniform(part_splits[11], (HORIZON, NU), jnp.float32) ** block_scale(part_splits[11], (HORIZON, NU), ((0, 64),), -0.2, 0.2), 0.1, 0.3)
    states = noise(part_splits[12], (HORIZON, NS), 0.03, 0.18, ((0, 64),), jnp.float32)
    inputs = noise(part_splits[13], (HORIZON, NU), 0.03, 0.18, ((0, 64),), jnp.float32)
    multipliers = noise(part_splits[14], (HORIZON, NS), 0.03, 0.18, ((0, 64),), jnp.float32)
    bound_mult = jnp.clip(0.06 * jax.random.uniform(part_splits[15], (HORIZON, NU), jnp.float32) ** block_scale(part_splits[15], (HORIZON, NU), ((0, 64),), -0.2, 0.2), 0.0, 0.06)
    active = with_ends((jax.random.randint(part_splits[16], (HORIZON, NU), 0, 3) < 1).astype(jnp.int32), jax.random.fold_in(part_splits[16], 1), 0, 1)
    return dict(state_map=state_map, input_map=input_map, closed_loop=closed_loop, feedback=feedback, value_matrix=value_matrix, gain_inverse=gain_inverse, input_weight=input_weight, state_weight=state_weight, state_linear=state_linear, input_linear=input_linear, offset=offset, upper_bound=upper_bound, states=states, inputs=inputs, multipliers=multipliers, bound_mult=bound_mult, active=active)


PRECISE = lax.Precision.HIGHEST
floor_share = 0.001

def apply_each(matrices, vectors):
    return jnp.einsum('kij,kj->ki', matrices, vectors, precision=PRECISE)

def apply_transposed(matrices, vectors):
    return jnp.einsum('kji,kj->ki', matrices, vectors, precision=PRECISE)

def backward_sweep(loop_mats, sources, incoming):

    def section(costate, section_item):
        matrix, source = section_item
        earlier = jnp.dot(costate, matrix, precision=PRECISE) + source
        return (earlier, (costate, earlier))
    final_state, (after, before) = lax.scan(section, incoming, (loop_mats, sources), reverse=True)
    return (after, before, final_state)

def forward_sweep(loop_mats, defects, pushes, entering):

    def section(carried, section_item):
        matrix, defect, pushed = section_item
        correction = carried - defect
        return (jnp.dot(matrix, correction, precision=PRECISE) + pushed, correction)
    final_state, steps = lax.scan(section, entering, (loop_mats, defects, pushes))
    return (steps, final_state)

def make_statistics(defect, grad_state, grad_input, slack_gap, offset, state_linear, input_linear, bound_mult):
    return jnp.stack([jnp.sum(defect * defect), jnp.sum(grad_state * grad_state) + jnp.sum(grad_input * grad_input), jnp.sum(slack_gap * slack_gap), jnp.sum(offset * offset), jnp.sum(state_linear * state_linear) + jnp.sum(input_linear * input_linear), jnp.sum(bound_mult * bound_mult)])

def make_norms(totals, horizon, state_count, input_count):
    primal = totals[0] / (totals[3] + floor_share * horizon * state_count)
    dual = totals[1] / (totals[4] + floor_share * horizon * (state_count + input_count))
    complement = totals[2] / (totals[5] + floor_share * horizon * input_count)
    return jnp.sqrt(jnp.stack([primal, dual, complement]))

def reference(state_map, input_map, closed_loop, feedback, value_matrix, gain_inverse, input_weight, state_weight, state_linear, input_linear, offset, upper_bound, states, inputs, multipliers, bound_mult, active):
    state_count = states.shape[1]
    input_count = inputs.shape[1]
    horizon = states.shape[0]
    predicted = apply_each(state_map, states) + apply_transposed(input_map, inputs)
    previous = jnp.concatenate([jnp.zeros((1, state_count), jnp.float32), predicted[:-1]], axis=0)
    defect = states - previous - offset
    following = jnp.concatenate([multipliers[1:], jnp.zeros((1, state_count), jnp.float32)], axis=0)
    grad_state = state_weight * states + state_linear + multipliers - apply_transposed(state_map, following)
    grad_input = jnp.einsum('ij,kj->ki', input_weight, inputs, precision=PRECISE) + input_linear - apply_each(input_map, following) + bound_mult
    slack_gap = bound_mult * (upper_bound - inputs)
    sources = apply_each(value_matrix, defect) + grad_state + apply_transposed(feedback, grad_input)
    after, before, unused = backward_sweep(closed_loop, sources, jnp.zeros((state_count,), jnp.float32))
    pulled = apply_each(input_map, after)
    forward_gain = -apply_each(gain_inverse, grad_input + pulled)
    pushes = apply_transposed(input_map, forward_gain)
    state_step, unused_final = forward_sweep(closed_loop, defect, pushes, jnp.zeros((state_count,), jnp.float32))
    chosen = active.astype(jnp.float32)
    input_step = (1.0 - chosen) * (apply_each(feedback, state_step) + forward_gain) + chosen * (upper_bound - inputs)
    multiplier_step = apply_each(value_matrix, state_step - defect) + before
    bound_step = chosen * (grad_input + jnp.einsum('ij,kj->ki', input_weight, input_step, precision=PRECISE) + pulled)
    totals = make_statistics(defect, grad_state, grad_input, slack_gap, offset, state_linear, input_linear, bound_mult)
    kkt_norms = make_norms(totals, horizon, state_count, input_count)
    return (state_step, input_step, multiplier_step, bound_step, kkt_norms)
```

```python
import jax
import jax.numpy as jnp
from jax import lax
from jax.experimental import pallas as pl
from jax.experimental.pallas import tpu as pltpu
from jax.sharding import Mesh
from jax.sharding import PartitionSpec as P

TM = ("tm_0", "tm_1", "tm_2")
BATCH_TM = ("batch", "tm_0", "tm_1", "tm_2")
MESH = pl.DeviceIdType.MESH
F32 = jnp.float32
BF16 = jnp.bfloat16
PRECISE = lax.Precision.HIGHEST
floor_share = 0.001
LINE = 4
HALF = 128


def split(a):
    high = a.astype(BF16)
    return high, (a - high.astype(F32)).astype(BF16)


def mm(a, b, ca=1, cb=0):
    dims = (((ca,), (cb,)), ((), ()))
    ah, al = split(a)
    bh, bl = split(b)
    dot = lambda x, y: lax.dot_general(x, y, dims, preferred_element_type=F32)
    return dot(ah, bh) + dot(ah, bl) + dot(al, bh)


def fold(t):
    return t[:, :HALF] + t[:, HALF:] if t.shape[1] > HALF else t


def across(t):
    return jnp.sum(jnp.transpose(t), axis=0, keepdims=True)


def row_mv(w, x):
    return across(fold(w * x))


def as_column(v):
    return jnp.transpose(jnp.broadcast_to(v, (HALF, v.shape[1])))


def col_apply(vc, w):
    n = w.shape[1]
    if n > HALF:
        vc = jnp.concatenate([vc] * (n // HALF), axis=1)
    else:
        vc = vc[:, :n]
    return jnp.sum(vc * w, axis=0, keepdims=True)


def col_mv(v, w):
    return col_apply(as_column(v), w)


def identity_matrix(n):
    i = lax.broadcasted_iota(jnp.int32, (n, n), 0)
    j = lax.broadcasted_iota(jnp.int32, (n, n), 1)
    return jnp.where(i == j, 1.0, 0.0).astype(F32)


def line_products(maps, suffix, prefix):
    n = maps.shape[1]
    upper = mm(maps[3], maps[2])
    lower = mm(maps[1], maps[0])
    suffix[1] = upper
    prefix[2] = lower
    return mm(upper, lower)


def line_rest(maps, suffix, prefix):
    eye = identity_matrix(maps.shape[1])
    suffix[3] = eye
    prefix[0] = eye
    suffix[2] = maps[3]
    prefix[1] = maps[0]
    suffix[0] = mm(suffix[1], maps[1])
    prefix[3] = mm(maps[2], prefix[2])


def kernel(
    state_map_h, input_map_h, closed_loop_h, feedback_h, value_h, gain_h, weight_h,
    state_weight_h, state_linear_h, input_linear_h, offset_h, upper_h, states_h, inputs_h,
    multipliers_h, bound_h, active_h,
    state_step, input_step, multiplier_step, bound_step, norms_out,
    sm, bm, am, fm, vm, gm, iw, state_weight, state_linear, input_linear, offset, upper,
    states, inputs, mult, bound, active,
    rst, qt, phi, mmat, wst, gwst,
    gz, gx, sz, pz, sx, px, omega, tback, tforw,
    predicted, following, defect, grad_state, grad_input, sources, after, pulled, gain, pushes,
    from_next, from_prev, cz, cx, fz, fx, vy, xy, dy, ey, sy,
    vloc_z, vloc_x, xloc_z, xloc_x, cvec,
    in_sem, a_sem, m_send, m_recv, v_send, v_recv, e_send, e_recv,
):
    count, ns = states.shape
    nu = inputs.shape[1]
    y, x, z = (lax.axis_index(a) for a in TM)
    place = (y * LINE + x) * LINE + z
    last = LINE**3 - 1

    def device_at(index):
        return {
            "tm_0": lax.div(index, LINE * LINE),
            "tm_1": lax.rem(lax.div(index, LINE), LINE),
            "tm_2": lax.rem(index, LINE),
        }

    next_device = device_at(lax.rem(place + 1, last + 1))
    prev_device = device_at(lax.rem(place + last, last + 1))
    spot = {"tm_0": y, "tm_1": x, "tm_2": z}

    def peer(axis, by):
        return {axis: lax.rem(spot[axis] + by, LINE)}

    a_copies = [pltpu.make_async_copy(closed_loop_h.at[k], am.at[k], a_sem.at[k]) for k in range(count)]
    for i in range(count // 2):
        a_copies[count - 1 - i].start()
        a_copies[i].start()
    pairs = [
        (states_h, states), (inputs_h, inputs), (multipliers_h, mult), (input_map_h, bm),
        (state_map_h, sm), (state_weight_h, state_weight), (state_linear_h, state_linear),
        (input_linear_h, input_linear), (offset_h, offset), (upper_h, upper), (bound_h, bound),
        (active_h, active), (weight_h, iw), (value_h, vm), (feedback_h, fm), (gain_h, gm),
    ]
    in_copies = [pltpu.make_async_copy(s, d, in_sem.at[n]) for n, (s, d) in enumerate(pairs)]
    for copy in in_copies:
        copy.start()

    barrier = pltpu.get_barrier_semaphore()
    for axis in TM:
        for by in range(1, LINE):
            pl.semaphore_signal(barrier, inc=1, device_id=peer(axis, by), device_id_type=MESH)
    for device in (next_device, prev_device):
        pl.semaphore_signal(barrier, inc=1, device_id=device, device_id_type=MESH)

    top = count - 1
    a_copies[top].wait()
    a_copies[0].wait()
    rst[top - 1] = am[top]
    qt[1] = jnp.transpose(am[0])

    def chain_step(i):
        rst[top - 1 - i] = mm(rst[top - i], am[top - i])
        qt[i + 1] = mm(qt[i], am[i], 1, 1)

    mid = count // 2
    for i in range(1, mid):
        a_copies[top - i].wait()
        a_copies[i].wait()
    pl.loop(1, mid)(chain_step)
    whole = mm(rst[mid - 1], qt[mid], 1, 1)
    phi[...] = whole
    gz[z] = whole

    pl.semaphore_wait(barrier, 3 * (LINE - 1) + 2)

    def remote(src, dst, send, recv, device):
        return pltpu.make_async_remote_copy(
            src_ref=src, dst_ref=dst, send_sem=send, recv_sem=recv, device_id=device, device_id_type=MESH
        )

    high, low = pl.ds(0, ns // 2), pl.ds(ns // 2, ns // 2)

    def gather_maps(stage, axis, maps):
        at = spot[axis]
        right, left = peer(axis, 1), peer(axis, LINE - 1)
        before, behind = lax.rem(at + LINE - 1, LINE), lax.rem(at + 1, LINE)
        plan = [
            (at, high, right), (at, low, left), (at, low, right), (at, high, left),
            (before, high, right), (behind, low, left),
        ]
        return [
            remote(maps.at[s, rows], maps.at[s, rows], m_send.at[stage, n], m_recv.at[stage, n], dev)
            for n, (s, rows, dev) in enumerate(plan)
        ]

    def relay(copies):
        copies[0].wait_recv()
        copies[4].start()
        copies[1].wait_recv()
        copies[5].start()

    def finish(copies):
        for copy in copies[2:]:
            copy.wait_recv()
        for copy in copies:
            copy.wait_send()

    def gather_vectors(stage, axis, buf):
        at = spot[axis]
        return [
            remote(buf.at[at], buf.at[at], v_send.at[stage, by - 1], v_recv.at[stage, by - 1], peer(axis, by))
            for by in range(1, LINE)
        ]

    def run(copies):
        for copy in copies:
            copy.start()

    def wait(copies):
        for copy in copies:
            copy.wait_recv()
        for copy in copies:
            copy.wait_send()

    z_maps = gather_maps(0, "tm_2", gz)
    run(z_maps[:4])

    for copy in in_copies[:5]:
        copy.wait()
    to_prev = remote(mult.at[pl.ds(0, 8)], from_next, e_send.at[0], e_recv.at[0], prev_device)
    to_prev.start()

    for i in range(mid, top):
        pass
    pl.loop(mid, top)(chain_step)

    def predict(k):
        at = pl.ds(k, 1)
        predicted[at, :] = row_mv(sm[k], states[at, :]) + col_mv(inputs[at, :], bm[k])

    pl.loop(0, count)(predict)
    to_next = remote(predicted.at[pl.ds(count - 8, 8)], from_prev, e_send.at[1], e_recv.at[1], next_device)
    to_next.start()
    relay(z_maps)

    to_prev.wait_recv()
    following[pl.ds(0, count - 1), :] = mult[pl.ds(1, count - 1), :]
    following[pl.ds(count - 1, 1), :] = jnp.where(place == last, 0.0, from_next[pl.ds(0, 1), :])
    for copy in in_copies[5:]:
        copy.wait()

    def gradients(k):
        at = pl.ds(k, 1)
        ahead = following[at, :]
        grad_state[at, :] = col_mv(ahead, sm[k])
        grad_input[at, :] = row_mv(bm[k], ahead)

    pl.loop(0, count)(gradients)
    grad_state[...] = state_weight[...] * states[...] + state_linear[...] + mult[...] - grad_state[...]
    weighted = lax.dot_general(
        inputs[...], iw[...], (((1,), (1,)), ((), ())), precision=PRECISE, preferred_element_type=F32
    )
    grad_input[...] = weighted + input_linear[...] - grad_input[...] + bound[...]

    to_next.wait_recv()
    defect[pl.ds(1, count - 1), :] = (
        states[pl.ds(1, count - 1), :] - predicted[pl.ds(0, count - 1), :] - offset[pl.ds(1, count - 1), :]
    )
    entered = jnp.where(place == 0, 0.0, from_prev[pl.ds(7, 1), :])
    defect[pl.ds(0, 1), :] = states[pl.ds(0, 1), :] - entered - offset[pl.ds(0, 1), :]

    def source(k):
        at = pl.ds(k, 1)
        sources[at, :] = row_mv(vm[k], defect[at, :]) + grad_state[at, :] + col_mv(grad_input[at, :], fm[k])

    pl.loop(0, count)(source)

    def gather_source(k, acc):
        return acc + fold(qt[k] * sources[pl.ds(k, 1), :])

    acc = lax.fori_loop(1, count, gather_source, jnp.zeros((ns, HALF), F32))
    local_costate = across(acc) + sources[pl.ds(0, 1), :]
    cvec[pl.ds(0, 1), :] = local_costate

    slack = bound[...] * (upper[...] - inputs[...])
    lane = lax.broadcasted_iota(jnp.int32, (1, ns), 1)
    squares = lambda t: jnp.sum(t * t)
    sums = [
        squares(defect[...]), squares(grad_state[...]) + squares(grad_input[...]), squares(slack),
        squares(offset[...]), squares(state_linear[...]) + squares(input_linear[...]), squares(bound[...]),
    ]
    stats = jnp.zeros((1, ns), F32)
    for n, s in enumerate(sums):
        stats = jnp.where(lane == n, s, stats)

    cz[z, pl.ds(0, 1), :] = local_costate
    cz[z, pl.ds(1, 1), :] = stats
    cz[z, pl.ds(2, 6), :] = jnp.zeros((6, ns), F32)
    c_line = gather_vectors(0, "tm_2", cz)
    run(c_line)

    finish(z_maps)
    group = line_products(gz, sz, pz)
    gx[x] = group
    x_maps = gather_maps(1, "tm_1", gx)
    run(x_maps[:4])

    def backward(i, v):
        k = top - i
        after[pl.ds(k, 1), :] = v
        return col_mv(v, am[k]) + sources[pl.ds(k, 1), :]

    lax.fori_loop(0, count, backward, jnp.zeros((1, ns), F32))

    def respond(k):
        at = pl.ds(k, 1)
        pull = row_mv(bm[k], after[at, :])
        pulled[at, :] = pull
        step = -row_mv(gm[k], grad_input[at, :] + pull)
        gain[at, :] = step
        pushes[at, :] = col_mv(step, bm[k])

    pl.loop(0, count)(respond)

    def gather_push(k, acc):
        return acc + fold(rst[k] * (pushes[pl.ds(k, 1), :] - defect[pl.ds(k + 1, 1), :]))

    acc = lax.fori_loop(0, top, gather_push, -fold(phi[...] * defect[pl.ds(0, 1), :]))
    f_zero = across(acc) + pushes[pl.ds(top, 1), :]

    relay(x_maps)

    def reach(k):
        w = mm(bm[k], rst[k], 1, 1)
        rows = pl.ds(pl.multiple_of(k * nu, nu), nu)
        wst[rows, :] = w
        gwst[rows, :] = mm(gm[k], w)

    pl.loop(0, top)(reach)
    wst[pl.ds(top * nu, nu), :] = bm[top]
    gwst[pl.ds(top * nu, nu), :] = mm(gm[top], bm[top])
    mmat[...] = mm(wst[...], gwst[...], 0, 0)

    line_rest(gz, sz, pz)
    wait(c_line)

    def line_backward(buf, maps, store):
        v = buf[LINE - 1, pl.ds(0, 1), :]
        store[LINE - 1] = jnp.zeros((8, ns), F32)
        for p in reversed(range(LINE - 1)):
            store[p] = jnp.broadcast_to(v, (8, ns))
            v = col_mv(v, maps[p]) + buf[p, pl.ds(0, 1), :]
        total = jnp.sum(buf[:, 1:2, :], axis=0)
        return v, total

    group_costate, totals = line_backward(cz, gz, vloc_z)
    cx[x, pl.ds(0, 1), :] = group_costate
    cx[x, pl.ds(1, 1), :] = totals
    cx[x, pl.ds(2, 6), :] = jnp.zeros((6, ns), F32)
    cx_line = gather_vectors(1, "tm_1", cx)
    run(cx_line)
    wait(cx_line)

    finish(x_maps)
    omega[...] = line_products(gx, sx, px)
    plane_costate, totals = line_backward(cx, gx, vloc_x)
    sy[y] = jnp.broadcast_to(totals, (8, ns))
    s_line = gather_vectors(4, "tm_0", sy)
    run(s_line)
    line_rest(gx, sx, px)
    tback[...] = mm(sx[x], sz[z])
    tforw[...] = mm(pz[z], px[x])
    t_zero = col_mv(vloc_x[x, pl.ds(0, 1), :], sz[z]) + vloc_z[z, pl.ds(0, 1), :]

    down = remote(dy, vy, e_send.at[2], e_recv.at[2], peer("tm_0", LINE - 1))

    @pl.when(y == LINE - 1)
    def _():
        vy[...] = jnp.zeros((8, ns), F32)

    @pl.when(y < LINE - 1)
    def _():
        down.wait_recv()

    plane_in = vy[pl.ds(0, 1), :]

    @pl.when(y > 0)
    def _():
        dy[...] = jnp.broadcast_to(col_mv(plane_in, omega[...]) + plane_costate, (8, ns))
        down.start()

    v = col_mv(plane_in, tback[...]) + t_zero
    f_own = f_zero - row_mv(mmat[...], v)
    fz[z] = jnp.broadcast_to(f_own, (8, ns))
    f_line = gather_vectors(2, "tm_2", fz)
    run(f_line)

    vc = as_column(v)

    def lift(k):
        at = pl.ds(k, 1)
        after[at, :] = after[at, :] + col_apply(vc, rst[k])

    pl.loop(0, top)(lift)
    after[pl.ds(top, 1), :] = v
    before_first = col_apply(vc, phi[...]) + cvec[pl.ds(0, 1), :]

    def line_forward(buf, suffix):
        acc = jnp.zeros((ns, HALF), F32)
        for p in range(LINE):
            acc = acc + fold(suffix[p] * buf[p, pl.ds(0, 1), :])
        return across(acc)

    def line_states(buf, maps, store):
        store[0] = jnp.zeros((8, ns), F32)
        v = buf[0, pl.ds(0, 1), :]
        store[1] = jnp.broadcast_to(v, (8, ns))
        for p in range(1, LINE - 1):
            v = row_mv(maps[p], v) + buf[p, pl.ds(0, 1), :]
            store[p + 1] = jnp.broadcast_to(v, (8, ns))

    wait(f_line)
    fx[x] = jnp.broadcast_to(line_forward(fz, sz), (8, ns))
    fx_line = gather_vectors(3, "tm_1", fx)
    run(fx_line)

    pl.loop(0, count)(respond)

    wait(fx_line)
    plane_state = line_forward(fx, sx)

    up = remote(ey, xy, e_send.at[3], e_recv.at[3], peer("tm_0", 1))

    def pass_up():
        entering = xy[pl.ds(0, 1), :]
        ey[...] = jnp.broadcast_to(row_mv(omega[...], entering) + plane_state, (8, ns))
        up.start()

    @pl.when(y == 0)
    def _():
        xy[...] = jnp.zeros((8, ns), F32)
        ey[...] = jnp.broadcast_to(plane_state, (8, ns))
        up.start()

    line_states(fz, gz, xloc_z)
    line_states(fx, gx, xloc_x)
    x_zero = row_mv(pz[z], xloc_x[x, pl.ds(0, 1), :]) + xloc_z[z, pl.ds(0, 1), :]

    def forward(k, carried):
        correction = carried - defect[pl.ds(k, 1), :]
        state_step[pl.ds(k, 1), :] = correction
        return row_mv(am[k], correction) + pushes[pl.ds(k, 1), :]

    @pl.when(y > 0)
    def _():
        up.wait_recv()

    @pl.when((y > 0) & (y < LINE - 1))
    def _():
        pass_up()

    lax.fori_loop(0, count, forward, jnp.zeros((1, ns), F32))

    x_in = row_mv(tforw[...], xy[pl.ds(0, 1), :]) + x_zero
    xc = as_column(x_in)
    state_step[pl.ds(0, 1), :] = state_step[pl.ds(0, 1), :] + x_in

    def settle(k):
        at = pl.ds(k, 1)
        state_step[at, :] = state_step[at, :] + col_apply(xc, qt[k])

    pl.loop(1, count)(settle)

    def close(k):
        at = pl.ds(k, 1)
        here = state_step[at, :]
        multiplier_step[at, :] = row_mv(vm[k], here - defect[at, :])
        input_step[at, :] = row_mv(fm[k], here)

    pl.loop(0, count)(close)
    multiplier_step[pl.ds(1, count - 1), :] = (
        multiplier_step[pl.ds(1, count - 1), :] + after[pl.ds(0, count - 1), :]
    )
    multiplier_step[pl.ds(0, 1), :] = multiplier_step[pl.ds(0, 1), :] + before_first
    chosen = active[...].astype(F32)
    step = (1.0 - chosen) * (input_step[...] + gain[...]) + chosen * (upper[...] - inputs[...])
    input_step[...] = step
    weighted = lax.dot_general(
        step, iw[...], (((1,), (1,)), ((), ())), precision=PRECISE, preferred_element_type=F32
    )
    bound_step[...] = chosen * (grad_input[...] + weighted + pulled[...])

    wait(s_line)
    totals = jnp.sum(sy[:, 0:1, :], axis=0)
    horizon = count * LINE**3
    pick = lambda n: jnp.sum(jnp.where(lane == n, totals, 0.0), axis=1, keepdims=True)
    primal = pick(0) / (pick(3) + floor_share * horizon * ns)
    dual = pick(1) / (pick(4) + floor_share * horizon * (ns + nu))
    complement = pick(2) / (pick(5) + floor_share * horizon * nu)
    lanes = lax.broadcasted_iota(jnp.int32, norms_out.shape, 1)
    values = jnp.where(lanes == 0, primal, jnp.where(lanes == 1, dual, complement))
    norms_out[...] = jnp.sqrt(values)

    to_prev.wait_send()
    to_next.wait_send()

    @pl.when(y > 0)
    def _():
        down.wait_send()

    @pl.when(y < LINE - 1)
    def _():
        up.wait_send()


def local(*args):
    states, inputs = args[12], args[13]
    count, ns = states.shape
    nu = inputs.shape[1]
    v = lambda *shape: pltpu.VMEM(shape, F32)
    dma = lambda *shape: pltpu.SemaphoreType.DMA(shape)
    scratch = [
        v(count, ns, ns), v(count, nu, ns), v(count, ns, ns), v(count, nu, ns), v(count, ns, ns),
        v(count, nu, nu), v(nu, nu), v(count, ns), v(count, ns), v(count, nu), v(count, ns), v(count, nu),
        v(count, ns), v(count, nu), v(count, ns), v(count, nu), pltpu.VMEM((count, nu), jnp.int32),
        v(count, ns, ns), v(count, ns, ns), v(ns, ns), v(ns, ns), v(count * nu, ns), v(count * nu, ns),
        v(LINE, ns, ns), v(LINE, ns, ns), v(LINE, ns, ns), v(LINE, ns, ns), v(LINE, ns, ns), v(LINE, ns, ns),
        v(ns, ns), v(ns, ns), v(ns, ns),
        v(count, ns), v(count, ns), v(count, ns), v(count, ns), v(count, nu), v(count, ns), v(count, ns),
        v(count, nu), v(count, nu), v(count, ns),
        v(8, ns), v(8, ns), v(LINE, 8, ns), v(LINE, 8, ns), v(LINE, 8, ns), v(LINE, 8, ns),
        v(8, ns), v(8, ns), v(8, ns), v(8, ns), v(LINE, 8, ns),
        v(LINE, 8, ns), v(LINE, 8, ns), v(LINE, 8, ns), v(LINE, 8, ns), v(8, ns),
        dma(16), dma(count), dma(2, 6), dma(2, 6), dma(5, LINE - 1), dma(5, LINE - 1), dma(4), dma(4),
    ]
    vmem = pl.BlockSpec(memory_space=pltpu.VMEM)
    out = pl.pallas_call(
        kernel,
        out_shape=[
            jax.ShapeDtypeStruct((count, ns), F32),
            jax.ShapeDtypeStruct((count, nu), F32),
            jax.ShapeDtypeStruct((count, ns), F32),
            jax.ShapeDtypeStruct((count, nu), F32),
            jax.ShapeDtypeStruct((8, HALF), F32),
        ],
        in_specs=[pl.BlockSpec(memory_space=pl.ANY)] * len(args),
        out_specs=[vmem] * 5,
        scratch_shapes=scratch,
        compiler_params=pltpu.CompilerParams(
            collective_id=0, has_side_effects=True, vmem_limit_bytes=60 * 1024 * 1024
        ),
        name="riccati",
    )(*args)
    return (*out[:4], out[4][0, :3])


def solution(mesh):
    lines = Mesh(
        mesh.devices.reshape(LINE, LINE, LINE, mesh.shape["batch"]), ("tm_0", "tm_1", "tm_2", "batch")
    )
    cube, flat = P(BATCH_TM, None, None), P(BATCH_TM, None)
    return jax.shard_map(
        local,
        mesh=lines,
        in_specs=(cube,) * 6 + (P("batch", None),) + (flat,) * 10,
        out_specs=(flat, flat, flat, flat, P("batch")),
        check_vma=False,
    )
```

```python
import jax
import jax.numpy as jnp
from jax import lax
from jax.experimental import pallas as pl
from jax.experimental.pallas import tpu as pltpu
from jax.sharding import Mesh
from jax.sharding import PartitionSpec as P

TM = ("tm_0", "tm_1", "tm_2")
BATCH_TM = ("batch", "tm_0", "tm_1", "tm_2")
MESH = pl.DeviceIdType.MESH
F32 = jnp.float32
BF16 = jnp.bfloat16
PRECISE = lax.Precision.HIGHEST
floor_share = 0.001
LINE = 4
HALF = 128


def split(a):
    high = a.astype(BF16)
    return high, (a - high.astype(F32)).astype(BF16)


def mm(a, b, ca=1, cb=0):
    dims = (((ca,), (cb,)), ((), ()))
    ah, al = split(a)
    bh, bl = split(b)
    dot = lambda x, y: lax.dot_general(x, y, dims, preferred_element_type=F32)
    return dot(ah, bh) + dot(ah, bl) + dot(al, bh)


def fold(t):
    return t[:, :HALF] + t[:, HALF:] if t.shape[1] > HALF else t


def across(t):
    return jnp.sum(jnp.transpose(t), axis=0, keepdims=True)


def row_mv(w, x):
    return across(fold(w * x))


def as_column(v):
    return jnp.transpose(jnp.broadcast_to(v, (HALF, v.shape[1])))


def col_apply(vc, w):
    n = w.shape[1]
    if n > HALF:
        vc = jnp.concatenate([vc] * (n // HALF), axis=1)
    else:
        vc = vc[:, :n]
    return jnp.sum(vc * w, axis=0, keepdims=True)


def col_mv(v, w):
    return col_apply(as_column(v), w)


def identity_matrix(n):
    i = lax.broadcasted_iota(jnp.int32, (n, n), 0)
    j = lax.broadcasted_iota(jnp.int32, (n, n), 1)
    return jnp.where(i == j, 1.0, 0.0).astype(F32)


def line_products(maps, suffix, prefix):
    n = maps.shape[1]
    upper = mm(maps[3], maps[2])
    lower = mm(maps[1], maps[0])
    suffix[1] = upper
    prefix[2] = lower
    return mm(upper, lower)


def line_rest(maps, suffix, prefix):
    eye = identity_matrix(maps.shape[1])
    suffix[3] = eye
    prefix[0] = eye
    suffix[2] = maps[3]
    prefix[1] = maps[0]
    suffix[0] = mm(suffix[1], maps[1])
    prefix[3] = mm(maps[2], prefix[2])


def kernel(
    state_map_h, input_map_h, closed_loop_h, feedback_h, value_h, gain_h, weight_h,
    state_weight_h, state_linear_h, input_linear_h, offset_h, upper_h, states_h, inputs_h,
    multipliers_h, bound_h, active_h,
    packed,
    sm, bm, am, fm, vm, gm, iw, state_weight, state_linear, input_linear, offset, upper,
    states, inputs, mult, bound, active,
    rst, qt, tree, phi, mmat, wst, gwst,
    gz, gx, sz, pz, sx, px, omega, om1, om2, tback, tforw,
    predicted, following, defect, grad_state, grad_input, sources, after, pulled, gain, pushes, state_step,
    edge, from_next, from_prev, cz, cx, plane, fy, vy, dy, sy,
    vloc_z, vloc_x, cvec,
    in_sem, a_sem, m_send, m_recv, v_send, v_recv, e_send, e_recv, p_send, p_recv, y_send, y_recv, f_send, f_recv,
):
    count, ns = states.shape
    nu = inputs.shape[1]
    y, x, z = (lax.axis_index(a) for a in TM)
    place = (y * LINE + x) * LINE + z
    last = LINE**3 - 1
    top = count - 1

    def device_at(index):
        return {
            "tm_0": lax.div(index, LINE * LINE),
            "tm_1": lax.rem(lax.div(index, LINE), LINE),
            "tm_2": lax.rem(index, LINE),
        }

    next_device = device_at(lax.rem(place + 1, last + 1))
    prev_device = device_at(lax.rem(place + last, last + 1))
    spot = {"tm_0": y, "tm_1": x, "tm_2": z}

    def peer(axis, by):
        return {axis: lax.rem(spot[axis] + by, LINE)}

    offsets = [(i, j) for i in range(LINE) for j in range(LINE) if i or j]

    def in_plane(i, j):
        return {"tm_1": lax.rem(x + i, LINE), "tm_2": lax.rem(z + j, LINE)}

    a_copies = [pltpu.make_async_copy(closed_loop_h.at[k], am.at[k], a_sem.at[k]) for k in range(count)]
    pairs = [
        (states_h, states), (inputs_h, inputs), (input_map_h.at[top], bm.at[top]), (state_map_h.at[top], sm.at[top]),
        (multipliers_h, mult), (input_map_h.at[pl.ds(0, top)], bm.at[pl.ds(0, top)]),
        (state_map_h.at[pl.ds(0, top)], sm.at[pl.ds(0, top)]), (state_weight_h, state_weight),
        (state_linear_h, state_linear), (input_linear_h, input_linear), (offset_h, offset), (upper_h, upper),
        (bound_h, bound), (active_h, active), (weight_h, iw), (value_h, vm), (feedback_h, fm), (gain_h, gm),
    ]
    in_copies = [pltpu.make_async_copy(s, d, in_sem.at[n]) for n, (s, d) in enumerate(pairs)]
    for copy in in_copies[:5]:
        copy.start()
    for copy in a_copies:
        copy.start()

    barrier = pltpu.get_barrier_semaphore()
    for by in range(1, LINE):
        pl.semaphore_signal(barrier, inc=1, device_id=peer("tm_0", by), device_id_type=MESH)
    for i, j in offsets:
        pl.semaphore_signal(barrier, inc=1, device_id=in_plane(i, j), device_id_type=MESH)
    for device in (next_device, prev_device):
        pl.semaphore_signal(barrier, inc=1, device_id=device, device_id_type=MESH)

    def predict(k):
        at = pl.ds(k, 1)
        predicted[at, :] = row_mv(sm[k], states[at, :]) + col_mv(inputs[at, :], bm[k])

    for copy in a_copies[: count // 2]:
        copy.wait()
    for i in range(count // 4):
        tree[i] = mm(am[2 * i + 1], am[2 * i])
    for copy in a_copies[count // 2 :] + in_copies[:5]:
        copy.wait()
    predict(top)
    edge[...] = jnp.broadcast_to(predicted[pl.ds(top, 1), :], (8, ns))
    for copy in in_copies[5:]:
        copy.start()
    for i in range(count // 4, count // 2):
        tree[i] = mm(am[2 * i + 1], am[2 * i])
    level = [tree[i] for i in range(count // 2)]
    while len(level) > 1:
        level = [mm(level[i + 1], level[i]) for i in range(0, len(level), 2)]
    phi[...] = level[0]
    gz[z] = level[0]

    pl.semaphore_wait(barrier, (LINE - 1) + len(offsets) + 2)

    def remote(src, dst, send, recv, device):
        return pltpu.make_async_remote_copy(
            src_ref=src, dst_ref=dst, send_sem=send, recv_sem=recv, device_id=device, device_id_type=MESH
        )

    high, low = pl.ds(0, ns // 2), pl.ds(ns // 2, ns // 2)

    def gather_maps(stage, axis, maps):
        at = spot[axis]
        right, left = peer(axis, 1), peer(axis, LINE - 1)
        before, behind = lax.rem(at + LINE - 1, LINE), lax.rem(at + 1, LINE)
        plan = [
            (at, high, right), (at, low, left), (at, low, right), (at, high, left),
            (before, high, right), (behind, low, left),
        ]
        return [
            remote(maps.at[s, rows], maps.at[s, rows], m_send.at[stage, n], m_recv.at[stage, n], dev)
            for n, (s, rows, dev) in enumerate(plan)
        ]

    def relay(copies):
        copies[0].wait_recv()
        copies[4].start()
        copies[1].wait_recv()
        copies[5].start()

    def gather_vectors(stage, axis, buf):
        at = spot[axis]
        return [
            remote(buf.at[at], buf.at[at], v_send.at[stage, by - 1], v_recv.at[stage, by - 1], peer(axis, by))
            for by in range(1, LINE)
        ]

    def run(copies):
        for copy in copies:
            copy.start()

    def arrive(copies):
        for copy in copies:
            copy.wait_recv()

    to_prev = remote(mult.at[pl.ds(0, 8)], from_next, e_send.at[0], e_recv.at[0], prev_device)
    to_next = remote(edge, from_prev, e_send.at[1], e_recv.at[1], next_device)
    z_maps = gather_maps(0, "tm_2", gz)
    run([to_prev, to_next] + z_maps[:4])

    half = count // 2
    rst[top - 1] = am[top]
    rst[top - 2] = tree[half - 1]
    qt[1] = jnp.transpose(am[0])
    qt[2] = jnp.transpose(tree[0])

    def chain_step(i):
        j = half - 1 - i
        suffix, prefix = rst[2 * j + 1], qt[2 * i]
        rst[2 * j] = mm(suffix, am[2 * j + 1])
        rst[2 * j - 1] = mm(suffix, tree[j])
        qt[2 * i + 1] = mm(prefix, am[2 * i], 1, 1)
        qt[2 * i + 2] = mm(prefix, tree[i], 1, 1)

    pl.loop(1, half - 1)(chain_step)
    rst[0] = mm(rst[1], am[1])
    qt[top] = mm(qt[top - 1], am[top - 1], 1, 1)

    for copy in in_copies[5:]:
        copy.wait()
    pl.loop(0, top, unroll=5)(predict)

    relay(z_maps)

    to_prev.wait_recv()
    following[pl.ds(0, top), :] = mult[pl.ds(1, top), :]
    following[pl.ds(top, 1), :] = jnp.where(place == last, 0.0, from_next[pl.ds(0, 1), :])

    def gradients(k):
        at = pl.ds(k, 1)
        ahead = following[at, :]
        grad_state[at, :] = col_mv(ahead, sm[k])
        grad_input[at, :] = row_mv(bm[k], ahead)

    pl.loop(0, count, unroll=4)(gradients)
    grad_state[...] = state_weight[...] * states[...] + state_linear[...] + mult[...] - grad_state[...]
    weighted = lax.dot_general(
        inputs[...], iw[...], (((1,), (1,)), ((), ())), precision=PRECISE, preferred_element_type=F32
    )
    grad_input[...] = weighted + input_linear[...] - grad_input[...] + bound[...]

    to_next.wait_recv()
    defect[pl.ds(1, top), :] = states[pl.ds(1, top), :] - predicted[pl.ds(0, top), :] - offset[pl.ds(1, top), :]
    entered = jnp.where(place == 0, 0.0, from_prev[pl.ds(0, 1), :])
    defect[pl.ds(0, 1), :] = states[pl.ds(0, 1), :] - entered - offset[pl.ds(0, 1), :]

    def source(k):
        at = pl.ds(k, 1)
        sources[at, :] = row_mv(vm[k], defect[at, :]) + grad_state[at, :] + col_mv(grad_input[at, :], fm[k])

    pl.loop(0, count, unroll=4)(source)

    def gather_source(k, acc):
        return acc + fold(qt[k] * sources[pl.ds(k, 1), :])

    acc = lax.fori_loop(1, count, gather_source, jnp.zeros((ns, HALF), F32), unroll=3)
    local_costate = across(acc) + sources[pl.ds(0, 1), :]
    cvec[pl.ds(0, 1), :] = local_costate

    slack = bound[...] * (upper[...] - inputs[...])
    lane = lax.broadcasted_iota(jnp.int32, (1, ns), 1)
    squares = lambda t: jnp.sum(t * t)
    sums = [
        squares(defect[...]), squares(grad_state[...]) + squares(grad_input[...]), squares(slack),
        squares(offset[...]), squares(state_linear[...]) + squares(input_linear[...]), squares(bound[...]),
    ]
    stats = jnp.zeros((1, ns), F32)
    for n, s in enumerate(sums):
        stats = jnp.where(lane == n, s, stats)

    cz[z, pl.ds(0, 1), :] = local_costate
    cz[z, pl.ds(1, 1), :] = stats
    cz[z, pl.ds(2, 6), :] = jnp.zeros((6, ns), F32)
    c_line = gather_vectors(0, "tm_2", cz)
    run(c_line)

    arrive(z_maps[2:])
    gx[x] = line_products(gz, sz, pz)
    x_maps = gather_maps(1, "tm_1", gx)

    def line_backward(buf, maps, store):
        v = buf[LINE - 1, pl.ds(0, 1), :]
        store[LINE - 1] = jnp.zeros((8, ns), F32)
        for p in reversed(range(LINE - 1)):
            store[p] = jnp.broadcast_to(v, (8, ns))
            v = col_mv(v, maps[p]) + buf[p, pl.ds(0, 1), :]
        total = jnp.sum(buf[:, 1:2, :], axis=0)
        return v, total

    run(x_maps[:4])

    def backward(i, v):
        k = top - i
        after[pl.ds(k, 1), :] = v
        return col_mv(v, am[k]) + sources[pl.ds(k, 1), :]

    lax.fori_loop(0, count, backward, jnp.zeros((1, ns), F32))

    arrive(c_line)
    group_costate, totals = line_backward(cz, gz, vloc_z)
    cx[x, pl.ds(0, 1), :] = group_costate
    cx[x, pl.ds(1, 1), :] = totals
    cx[x, pl.ds(2, 6), :] = jnp.zeros((6, ns), F32)
    cx_line = gather_vectors(1, "tm_1", cx)
    run(cx_line)

    def respond(k):
        at = pl.ds(k, 1)
        pull = row_mv(bm[k], after[at, :])
        pulled[at, :] = pull
        step = -row_mv(gm[k], grad_input[at, :] + pull)
        gain[at, :] = step
        pushes[at, :] = col_mv(step, bm[k])

    pl.loop(0, count, unroll=8)(respond)

    def gather_push(k, acc):
        return acc + fold(rst[k] * (pushes[pl.ds(k, 1), :] - defect[pl.ds(k + 1, 1), :]))

    acc = lax.fori_loop(0, top, gather_push, -fold(phi[...] * defect[pl.ds(0, 1), :]), unroll=3)
    f_zero = across(acc) + pushes[pl.ds(top, 1), :]

    relay(x_maps)

    def reach(k):
        w = mm(bm[k], rst[k], 1, 1)
        rows = pl.ds(pl.multiple_of(k * nu, nu), nu)
        wst[rows, :] = w
        gwst[rows, :] = mm(gm[k], w)

    pl.loop(0, top, unroll=5)(reach)
    wst[pl.ds(top * nu, nu), :] = bm[top]
    gwst[pl.ds(top * nu, nu), :] = mm(gm[top], bm[top])

    def gather_reach():
        mmat[...] = mm(wst[...], gwst[...], 0, 0)

    arrive(cx_line)

    arrive(x_maps[2:])
    plane_costate, totals = line_backward(cx, gx, vloc_x)

    down = remote(dy, vy, e_send.at[2], e_recv.at[2], peer("tm_0", LINE - 1))

    @pl.when(y == LINE - 1)
    def _():
        vy[...] = jnp.zeros((8, ns), F32)
        dy[...] = jnp.broadcast_to(plane_costate, (8, ns))
        down.start()

    omega[...] = line_products(gx, sx, px)

    second = [remote(omega.at[r], om1.at[r], y_send.at[n], y_recv.at[n], peer("tm_0", 1)) for n, r in enumerate((high, low))]
    third = [remote(omega.at[r], om2.at[r], y_send.at[2 + n], y_recv.at[2 + n], peer("tm_0", 1)) for n, r in enumerate((high, low))]
    passed = [remote(om1.at[r], om1.at[r], y_send.at[4 + n], y_recv.at[4 + n], peer("tm_0", 1)) for n, r in enumerate((high, low))]

    @pl.when(y == 1)
    def _():
        run(second)

    @pl.when(y == 2)
    def _():
        run(third)

    sy[y] = jnp.broadcast_to(totals, (8, ns))
    s_line = gather_vectors(2, "tm_0", sy)
    run(s_line)
    line_rest(gz, sz, pz)
    line_rest(gx, sx, px)
    tback[...] = mm(sx[x], sz[z])
    t_zero = col_mv(vloc_x[x, pl.ds(0, 1), :], sz[z]) + vloc_z[z, pl.ds(0, 1), :]

    pl.when(y == 0)(gather_reach)

    @pl.when(y < LINE - 1)
    def _():
        down.wait_recv()

    plane_in = vy[pl.ds(0, 1), :]

    @pl.when((y > 0) & (y < LINE - 1))
    def _():
        dy[...] = jnp.broadcast_to(col_mv(plane_in, omega[...]) + plane_costate, (8, ns))
        down.start()

    pl.when(y > 0)(gather_reach)

    v = col_mv(plane_in, tback[...]) + t_zero
    f_own = f_zero - row_mv(mmat[...], v)
    here = x * LINE + z
    plane[here, pl.ds(0, 1), :] = row_mv(tback[...], f_own)
    plane[here, pl.ds(1, 1), :] = row_mv(sz[z], f_own)
    plane[here, pl.ds(2, 1), :] = f_own
    plane[here, pl.ds(3, 1), :] = f_own
    rows = pl.ds(0, 4)
    plane_line = [
        remote(plane.at[here, rows], plane.at[here, rows], p_send.at[n], p_recv.at[n], in_plane(i, j))
        for n, (i, j) in enumerate(offsets)
    ]
    run(plane_line)

    vc = as_column(v)

    def lift(k):
        at = pl.ds(k, 1)
        after[at, :] = after[at, :] + col_apply(vc, rst[k])

    pl.loop(0, top, unroll=5)(lift)
    after[pl.ds(top, 1), :] = v
    before_first = col_apply(vc, phi[...]) + cvec[pl.ds(0, 1), :]

    pl.loop(0, count, unroll=8)(respond)

    arrive(plane_line)
    plane_state = jnp.sum(plane[:, 0:1, :], axis=0)
    fy[y] = jnp.broadcast_to(plane_state, (8, ns))
    ahead = [
        remote(fy.at[y], fy.at[y], f_send.at[by - 1], f_recv.at[by - 1], peer("tm_0", by)) for by in range(1, LINE)
    ]
    for by in range(1, LINE):
        @pl.when(y + by < LINE)
        def _(by=by):
            ahead[by - 1].start()

    @pl.when(y == 2)
    def _():
        for n in range(2):
            second[n].wait_recv()
            passed[n].start()

    def forward(k, carried):
        correction = carried - defect[pl.ds(k, 1), :]
        state_step[pl.ds(k, 1), :] = correction
        return row_mv(am[k], correction) + pushes[pl.ds(k, 1), :]

    lax.fori_loop(0, count, forward, jnp.zeros((1, ns), F32))

    tforw[...] = mm(pz[z], px[x])

    def line_state(vector, maps, at):
        entering = jnp.zeros((1, ns), F32)
        found = entering
        for p in range(LINE - 1):
            entering = row_mv(maps[p], entering) + vector(p) if p else vector(p)
            found = jnp.where(at == p + 1, entering, found)
        return found

    in_line = line_state(lambda p: plane[x * LINE + p, pl.ds(2, 1), :], gz, z)
    groups = [jnp.sum(plane[LINE * p : LINE * p + LINE, 1:2, :], axis=0) for p in range(LINE)]
    in_group = line_state(lambda p: groups[p], gx, x)
    x_zero = row_mv(pz[z], in_group) + in_line

    for by in range(1, LINE):
        @pl.when(y >= by)
        def _(by=by):
            ahead[by - 1].wait_recv()

    @pl.when(y == 0)
    def _():
        dy[...] = jnp.zeros((8, ns), F32)

    def enter(vector):
        dy[...] = jnp.broadcast_to(vector, (8, ns))

    at_plane = lambda p: fy[p, pl.ds(0, 1), :]

    @pl.when(y == 1)
    def _():
        down.wait_send()
        enter(at_plane(0))

    @pl.when(y == 2)
    def _():
        down.wait_send()
        enter(row_mv(om1[...], at_plane(0)) + at_plane(1))

    @pl.when(y == LINE - 1)
    def _():
        down.wait_send()
        arrive(third)
        arrive(passed)
        enter(row_mv(om2[...], row_mv(om1[...], at_plane(0)) + at_plane(1)) + at_plane(2))

    x_in = row_mv(tforw[...], dy[pl.ds(0, 1), :]) + x_zero
    xc = as_column(x_in)
    out_x, out_m = pl.ds(0, count), pl.ds(count, count)
    packed[pl.ds(0, 1), :] = state_step[pl.ds(0, 1), :] + x_in

    def settle(k):
        at = pl.ds(k, 1)
        packed[at, :] = state_step[at, :] + col_apply(xc, qt[k])

    pl.loop(1, count, unroll=5)(settle)

    def close(k):
        at = pl.ds(k, 1)
        now = packed[at, :]
        sources[at, :] = row_mv(vm[k], now - defect[at, :])
        input_linear[at, :] = row_mv(fm[k], now)

    pl.loop(0, count, unroll=8)(close)
    packed[pl.ds(count + 1, top), :] = sources[pl.ds(1, top), :] + after[pl.ds(0, top), :]
    packed[pl.ds(count, 1), :] = sources[pl.ds(0, 1), :] + before_first
    chosen = active[...].astype(F32)
    step = (1.0 - chosen) * (input_linear[...] + gain[...]) + chosen * (upper[...] - inputs[...])
    packed[pl.ds(2 * count, count), pl.ds(0, nu)] = step
    weighted = lax.dot_general(
        step, iw[...], (((1,), (1,)), ((), ())), precision=PRECISE, preferred_element_type=F32
    )
    packed[pl.ds(2 * count, count), pl.ds(HALF, nu)] = chosen * (grad_input[...] + weighted + pulled[...])

    arrive(s_line)
    totals = jnp.sum(sy[:, 0:1, :], axis=0)
    horizon = count * LINE**3
    pick = lambda n: jnp.sum(jnp.where(lane == n, totals, 0.0), axis=1, keepdims=True)
    primal = pick(0) / (pick(3) + floor_share * horizon * ns)
    dual = pick(1) / (pick(4) + floor_share * horizon * (ns + nu))
    complement = pick(2) / (pick(5) + floor_share * horizon * nu)
    lanes = lax.broadcasted_iota(jnp.int32, (8, ns), 1)
    values = jnp.where(lanes == 0, primal, jnp.where(lanes == 1, dual, complement))
    packed[pl.ds(3 * count, 8), :] = jnp.sqrt(values)

    for copy in [to_prev, to_next] + z_maps + x_maps + c_line + cx_line + plane_line + s_line:
        copy.wait_send()

    for by in range(1, LINE):
        @pl.when(y + by < LINE)
        def _(by=by):
            ahead[by - 1].wait_send()

    @pl.when(y == 1)
    def _():
        for copy in second:
            copy.wait_send()

    @pl.when(y == 2)
    def _():
        for copy in third + passed:
            copy.wait_send()


def unpack(packed, state_step, input_step, multiplier_step, bound_step, norms):
    count, nu = input_step.shape
    state_step[...] = packed[pl.ds(0, count), :]
    multiplier_step[...] = packed[pl.ds(count, count), :]
    input_step[...] = packed[pl.ds(2 * count, count), pl.ds(0, nu)]
    bound_step[...] = packed[pl.ds(2 * count, count), pl.ds(HALF, nu)]
    norms[...] = packed[pl.ds(3 * count, 1), pl.ds(0, HALF)][0, :3]


def local(*args):
    states, inputs = args[12], args[13]
    count, ns = states.shape
    nu = inputs.shape[1]
    v = lambda *shape: pltpu.VMEM(shape, F32)
    dma = lambda *shape: pltpu.SemaphoreType.DMA(shape)
    square = v(ns, ns)
    line = v(LINE, ns, ns)
    rows = v(LINE, 8, ns)
    row = v(8, ns)
    wide, narrow = v(count, ns), v(count, nu)
    scratch = [
        v(count, ns, ns), v(count, nu, ns), v(count, ns, ns), v(count, nu, ns), v(count, ns, ns),
        v(count, nu, nu), v(nu, nu), wide, wide, narrow, wide, narrow,
        wide, narrow, wide, narrow, pltpu.VMEM((count, nu), jnp.int32),
        v(count, ns, ns), v(count, ns, ns), v(count // 2, ns, ns), square, square, v(count * nu, ns), v(count * nu, ns),
        line, line, line, line, line, line, square, square, square, square, square,
        wide, wide, wide, wide, narrow, wide, wide, narrow, narrow, wide, wide,
        row, row, row, rows, rows, v(LINE * LINE, 8, ns), rows, row, row, rows,
        rows, rows, row,
        dma(18), dma(count), dma(2, 6), dma(2, 6), dma(3, LINE - 1), dma(3, LINE - 1), dma(3), dma(3),
        dma(LINE * LINE - 1), dma(LINE * LINE - 1), dma(6), dma(6), dma(LINE - 1), dma(LINE - 1),
    ]
    vmem = pl.BlockSpec(memory_space=pltpu.VMEM)
    packed = pl.pallas_call(
        kernel,
        out_shape=pltpu.VMEM((3 * count + 8, ns), F32),
        in_specs=[pl.BlockSpec(memory_space=pl.ANY)] * len(args),
        out_specs=vmem,
        scratch_shapes=scratch,
        compiler_params=pltpu.CompilerParams(
            collective_id=0, has_side_effects=True, vmem_limit_bytes=56 * 1024 * 1024
        ),
        name="riccati",
    )(*args)
    return pl.pallas_call(
        unpack,
        out_shape=[
            jax.ShapeDtypeStruct((count, ns), F32),
            jax.ShapeDtypeStruct((count, nu), F32),
            jax.ShapeDtypeStruct((count, ns), F32),
            jax.ShapeDtypeStruct((count, nu), F32),
            jax.ShapeDtypeStruct((3,), F32),
        ],
        in_specs=[vmem],
        out_specs=[vmem] * 5,
        name="unpack",
    )(pltpu.with_memory_space_constraint(packed, pltpu.VMEM))


def solution(mesh):
    lines = Mesh(
        mesh.devices.reshape(LINE, LINE, LINE, mesh.shape["batch"]), ("tm_0", "tm_1", "tm_2", "batch")
    )
    cube, flat = P(BATCH_TM, None, None), P(BATCH_TM, None)
    return jax.shard_map(
        local,
        mesh=lines,
        in_specs=(cube,) * 6 + (P("batch", None),) + (flat,) * 10,
        out_specs=(flat, flat, flat, flat, P("batch")),
        check_vma=False,
    )
```

```python
import jax
import jax.numpy as jnp
from jax import lax
from jax.experimental import pallas as pl
from jax.experimental.pallas import tpu as pltpu
from jax.sharding import Mesh
from jax.sharding import PartitionSpec as P

TM = ("tm_0", "tm_1", "tm_2")
BATCH_TM = ("batch", "tm_0", "tm_1", "tm_2")
MESH = pl.DeviceIdType.MESH
F32 = jnp.float32
BF16 = jnp.bfloat16
PRECISE = lax.Precision.HIGHEST
floor_share = 0.001
LINE = 4
HALF = 128


def split(a):
    high = a.astype(BF16)
    return high, (a - high.astype(F32)).astype(BF16)


def mm(a, b, ca=1, cb=0):
    dims = (((ca,), (cb,)), ((), ()))
    ah, al = split(a)
    bh, bl = split(b)
    dot = lambda x, y: lax.dot_general(x, y, dims, preferred_element_type=F32)
    return dot(ah, bh) + dot(ah, bl) + dot(al, bh)


def fold(t):
    return t[:, :HALF] + t[:, HALF:] if t.shape[1] > HALF else t


def across(t):
    return jnp.sum(jnp.transpose(t), axis=0, keepdims=True)


def row_mv(w, x):
    return across(fold(w * x))


def as_column(v):
    return jnp.transpose(jnp.broadcast_to(v, (HALF, v.shape[1])))


def col_apply(vc, w):
    n = w.shape[1]
    if n > HALF:
        vc = jnp.concatenate([vc] * (n // HALF), axis=1)
    else:
        vc = vc[:, :n]
    return jnp.sum(vc * w, axis=0, keepdims=True)


def col_mv(v, w):
    return col_apply(as_column(v), w)


def identity_matrix(n):
    i = lax.broadcasted_iota(jnp.int32, (n, n), 0)
    j = lax.broadcasted_iota(jnp.int32, (n, n), 1)
    return jnp.where(i == j, 1.0, 0.0).astype(F32)


def line_products(maps, suffix, prefix):
    n = maps.shape[1]
    upper = mm(maps[3], maps[2])
    lower = mm(maps[1], maps[0])
    suffix[1] = upper
    prefix[2] = lower
    return mm(upper, lower)


def line_rest(maps, suffix, prefix):
    eye = identity_matrix(maps.shape[1])
    suffix[3] = eye
    prefix[0] = eye
    suffix[2] = maps[3]
    prefix[1] = maps[0]
    suffix[0] = mm(suffix[1], maps[1])
    prefix[3] = mm(maps[2], prefix[2])


def kernel(
    state_map_h, input_map_h, closed_loop_h, feedback_h, value_h, gain_h, weight_h,
    state_weight_h, state_linear_h, input_linear_h, offset_h, upper_h, states_h, inputs_h,
    multipliers_h, bound_h, active_h,
    packed,
    sm, bm, am, fm, vm, gm, iw, state_weight, state_linear, input_linear, offset, upper,
    states, inputs, mult, bound, active,
    rst, qt, tree, phi, weighted_map, mmat, wst, gwst,
    gz, gx, sz, pz, sx, px, omega, om1, om2, tback, tforw,
    predicted, following, defect, grad_state, grad_input, sources, after, pulled, gain, pushes, state_step,
    edge, from_next, from_prev, cz, cx, plane_sum, plane_own, fy, vy, dy, entry, fvec, avec, answer, sy,
    vloc_z, vloc_x, cvec,
    in_sem, a_sem, m_send, m_recv, v_send, v_recv, e_send, e_recv, p_send, p_recv, y_send, y_recv, f_send, f_recv,
):
    count, ns = states.shape
    nu = inputs.shape[1]
    y, x, z = (lax.axis_index(a) for a in TM)
    core = lax.axis_index("batch")
    place = (y * LINE + x) * LINE + z
    last = LINE**3 - 1
    top = count - 1

    def device_at(index):
        return {
            "tm_0": lax.div(index, LINE * LINE),
            "tm_1": lax.rem(lax.div(index, LINE), LINE),
            "tm_2": lax.rem(index, LINE),
        }

    next_device = device_at(lax.rem(place + 1, last + 1))
    prev_device = device_at(lax.rem(place + last, last + 1))
    spot = {"tm_0": y, "tm_1": x, "tm_2": z}

    def peer(axis, by):
        return {axis: lax.rem(spot[axis] + by, LINE)}

    offsets = [(i, j) for i in range(LINE) for j in range(LINE) if i or j]

    def in_plane(i, j):
        return {"tm_1": lax.rem(x + i, LINE), "tm_2": lax.rem(z + j, LINE)}

    first_half, last_half = pl.ds(0, count // 2), pl.ds(count // 2, count // 2)
    a_copies = [
        pltpu.make_async_copy(closed_loop_h.at[k], am.at[k], a_sem.at[k // (count // 2)]) for k in range(count)
    ]
    a_halves = [
        pltpu.make_async_copy(closed_loop_h.at[part], am.at[part], a_sem.at[n])
        for n, part in enumerate((first_half, last_half))
    ]
    pairs = [
        (states_h, states), (inputs_h, inputs), (input_map_h.at[top], bm.at[top]), (state_map_h.at[top], sm.at[top]),
        (multipliers_h, mult), (input_map_h.at[pl.ds(0, top)], bm.at[pl.ds(0, top)]),
        (state_map_h.at[pl.ds(0, 8)], sm.at[pl.ds(0, 8)]),
        (state_map_h.at[pl.ds(8, top - 8)], sm.at[pl.ds(8, top - 8)]), (state_weight_h, state_weight),
        (state_linear_h, state_linear), (input_linear_h, input_linear), (offset_h, offset), (upper_h, upper),
        (bound_h, bound), (active_h, active), (weight_h, iw), (value_h, vm), (feedback_h, fm), (gain_h, gm),
    ]
    in_copies = [pltpu.make_async_copy(s, d, in_sem.at[n if n < 14 else n - 14]) for n, (s, d) in enumerate(pairs)]
    for copy in in_copies[:5]:
        copy.start()
    for copy in a_copies:
        copy.start()

    barrier = pltpu.get_barrier_semaphore()
    for by in range(1, LINE):
        pl.semaphore_signal(barrier, inc=1, device_id=peer("tm_0", by), device_id_type=MESH)
    for i, j in offsets:
        pl.semaphore_signal(barrier, inc=1, device_id=in_plane(i, j), device_id_type=MESH)
    for device in (next_device, prev_device):
        pl.semaphore_signal(barrier, inc=1, device_id=device, device_id_type=MESH)

    def predict(k):
        at = pl.ds(k, 1)
        predicted[at, :] = row_mv(sm[k], states[at, :]) + col_mv(inputs[at, :], bm[k])

    a_halves[0].wait()
    for i in range(count // 4):
        tree[i] = mm(am[2 * i + 1], am[2 * i])
    for copy in a_halves[1:] + in_copies[:5]:
        copy.wait()
    predict(top)
    edge[...] = jnp.broadcast_to(predicted[pl.ds(top, 1), :], (8, ns))
    for copy in in_copies[5:]:
        copy.start()
    for i in range(count // 4, count // 2):
        tree[i] = mm(am[2 * i + 1], am[2 * i])
    level = [tree[i] for i in range(count // 2)]
    while len(level) > 1:
        level = [mm(level[i + 1], level[i]) for i in range(0, len(level), 2)]
    phi[...] = level[0]
    gz[z] = level[0]

    pl.semaphore_wait(barrier, (LINE - 1) + len(offsets) + 2)

    def remote(src, dst, send, recv, device):
        return pltpu.make_async_remote_copy(
            src_ref=src, dst_ref=dst, send_sem=send, recv_sem=recv, device_id=device, device_id_type=MESH
        )

    part = ns // 4
    high, low = pl.ds(0, 2 * part), pl.ds(2 * part, 2 * part)
    quarters = [pl.ds(n * part, part) for n in range(4)]

    def gather_maps(stage, axis, maps):
        at = spot[axis]
        right, left = peer(axis, 1), peer(axis, LINE - 1)
        before, behind = lax.rem(at + LINE - 1, LINE), lax.rem(at + 1, LINE)
        plan = [
            (at, quarters[0], right), (at, quarters[3], left), (at, quarters[1], right), (at, quarters[2], left),
            (at, low, right), (at, high, left),
            (before, quarters[0], right), (behind, quarters[3], left),
            (before, quarters[1], right), (behind, quarters[2], left),
        ]
        sems = (0, 0, 1, 1, 2, 2, 2, 2, 2, 2)
        copies = [
            remote(maps.at[s, rows], maps.at[s, rows], m_send.at[stage], m_recv.at[stage, n], dev)
            for n, (s, rows, dev) in zip(sems, plan)
        ]
        whole = remote(maps.at[pl.ds(0, 3)], maps.at[pl.ds(0, 2)], m_send.at[stage], m_recv.at[stage, 2], right)
        return copies, whole

    def relay(copies, maps, stage, turn):
        remote(maps.at[0, high], maps.at[0, high], m_send.at[stage], m_recv.at[stage, turn], peer("tm_0", 1)).wait_recv()
        run(copies[2 * turn + 6 : 2 * turn + 8])

    def gather_vectors(stage, axis, buf):
        at = spot[axis]
        copies = [
            remote(buf.at[at], buf.at[at], v_send.at[stage], v_recv.at[stage], peer(axis, by)) for by in range(1, LINE)
        ]
        three = buf.at[pl.ds(0, LINE - 1)]
        return copies, remote(three, three, v_send.at[stage], v_recv.at[stage], peer(axis, 1))

    def run(copies):
        for copy in copies:
            copy.start()

    to_prev = remote(mult.at[pl.ds(0, 8)], from_next, e_send.at[0], e_recv.at[0], prev_device)
    to_next = remote(edge, from_prev, e_send.at[1], e_recv.at[1], next_device)
    z_maps, z_all = gather_maps(0, "tm_2", gz)
    run([to_prev, to_next])
    half = count // 2

    @pl.when(core == 0)
    def _():
        run(z_maps[:6])

    qt[1] = jnp.transpose(am[0])
    qt[2] = jnp.transpose(tree[0])

    def prefix_step(i):
        prefix = qt[2 * i]
        qt[2 * i + 1] = mm(prefix, am[2 * i], 1, 1)
        qt[2 * i + 2] = mm(prefix, tree[i], 1, 1)

    pl.loop(1, half - 1)(prefix_step)
    qt[top] = mm(qt[top - 1], am[top - 1], 1, 1)

    @pl.when(core == 0)
    def _():
        relay(z_maps, gz, 0, 0)

    for copy in in_copies[5:8]:
        copy.wait()
    pl.loop(0, top, unroll=5)(predict)

    @pl.when(core == 0)
    def _():
        relay(z_maps, gz, 0, 1)

    for copy in in_copies[8:16]:
        copy.wait()
    to_prev.wait_recv()
    following[pl.ds(0, top), :] = mult[pl.ds(1, top), :]
    following[pl.ds(top, 1), :] = jnp.where(place == last, 0.0, from_next[pl.ds(0, 1), :])

    def gradients(k):
        at = pl.ds(k, 1)
        ahead = following[at, :]
        grad_state[at, :] = col_mv(ahead, sm[k])
        grad_input[at, :] = row_mv(bm[k], ahead)

    pl.loop(0, count, unroll=4)(gradients)
    grad_state[...] = state_weight[...] * states[...] + state_linear[...] + mult[...] - grad_state[...]
    weighted = lax.dot_general(
        inputs[...], iw[...], (((1,), (1,)), ((), ())), precision=PRECISE, preferred_element_type=F32
    )
    grad_input[...] = weighted + input_linear[...] - grad_input[...] + bound[...]

    @pl.when(core == 1)
    def _():
        run(z_maps[:6])

    for copy in in_copies[16:]:
        copy.wait()
    to_next.wait_recv()
    defect[pl.ds(1, top), :] = states[pl.ds(1, top), :] - predicted[pl.ds(0, top), :] - offset[pl.ds(1, top), :]
    entered = jnp.where(place == 0, 0.0, from_prev[pl.ds(0, 1), :])
    defect[pl.ds(0, 1), :] = states[pl.ds(0, 1), :] - entered - offset[pl.ds(0, 1), :]

    def source(k):
        at = pl.ds(k, 1)
        sources[at, :] = row_mv(vm[k], defect[at, :]) + grad_state[at, :] + col_mv(grad_input[at, :], fm[k])
        weighted_map[k] = mm(gm[k], bm[k])

    pl.loop(0, count, unroll=4)(source)

    @pl.when(core == 1)
    def _():
        relay(z_maps, gz, 0, 0)
        relay(z_maps, gz, 0, 1)


    def gather_source(k, acc):
        return acc + fold(qt[k] * sources[pl.ds(k, 1), :])

    acc = lax.fori_loop(1, count, gather_source, jnp.zeros((ns, HALF), F32), unroll=3)
    local_costate = across(acc) + sources[pl.ds(0, 1), :]
    cvec[pl.ds(0, 1), :] = local_costate

    slack = bound[...] * (upper[...] - inputs[...])
    lane = lax.broadcasted_iota(jnp.int32, (1, ns), 1)
    squares = lambda t: jnp.sum(t * t)
    sums = [
        squares(defect[...]), squares(grad_state[...]) + squares(grad_input[...]), squares(slack),
        squares(offset[...]), squares(state_linear[...]) + squares(input_linear[...]), squares(bound[...]),
    ]
    stats = jnp.zeros((1, ns), F32)
    for n, s in enumerate(sums):
        stats = jnp.where(lane == n, s, stats)

    cz[z, pl.ds(0, 1), :] = local_costate
    cz[z, pl.ds(1, 1), :] = stats
    cz[z, pl.ds(2, 6), :] = jnp.zeros((6, ns), F32)
    c_line, c_all = gather_vectors(0, "tm_2", cz)
    run(c_line)

    z_all.wait_recv()
    gx[x] = line_products(gz, sz, pz)
    x_maps, x_all = gather_maps(1, "tm_1", gx)

    def line_backward(buf, maps, store):
        v = buf[LINE - 1, pl.ds(0, 1), :]
        store[LINE - 1] = jnp.zeros((8, ns), F32)
        for p in reversed(range(LINE - 1)):
            store[p] = jnp.broadcast_to(v, (8, ns))
            v = col_mv(v, maps[p]) + buf[p, pl.ds(0, 1), :]
        total = jnp.sum(buf[:, 1:2, :], axis=0)
        return v, total

    run(x_maps[:6])

    rst[top - 1] = am[top]
    rst[top - 2] = tree[half - 1]

    def suffix_step(i):
        j = half - 1 - i
        suffix = rst[2 * j + 1]
        rst[2 * j] = mm(suffix, am[2 * j + 1])
        rst[2 * j - 1] = mm(suffix, tree[j])

    pl.loop(1, half - 1)(suffix_step)
    rst[0] = mm(rst[1], am[1])

    c_all.wait_recv()
    group_costate, totals = line_backward(cz, gz, vloc_z)
    cx[x, pl.ds(0, 1), :] = group_costate
    cx[x, pl.ds(1, 1), :] = totals
    cx[x, pl.ds(2, 6), :] = jnp.zeros((6, ns), F32)
    cx_line, cx_all = gather_vectors(1, "tm_1", cx)
    run(cx_line)

    relay(x_maps, gx, 1, 0)

    def backward(i, v):
        k = top - i
        after[pl.ds(k, 1), :] = v
        return col_mv(v, am[k]) + sources[pl.ds(k, 1), :]

    v = lax.fori_loop(0, half, backward, jnp.zeros((1, ns), F32))
    relay(x_maps, gx, 1, 1)
    lax.fori_loop(half, count, backward, v)

    def respond(k):
        at = pl.ds(k, 1)
        pull = row_mv(bm[k], after[at, :])
        pulled[at, :] = pull
        step = -row_mv(gm[k], grad_input[at, :] + pull)
        gain[at, :] = step
        pushes[at, :] = col_mv(step, bm[k])

    def gather_push(k, acc):
        return acc + fold(rst[k] * (pushes[pl.ds(k, 1), :] - defect[pl.ds(k + 1, 1), :]))

    def local_state():
        pl.loop(0, count, unroll=8)(respond)
        acc = lax.fori_loop(0, top, gather_push, -fold(phi[...] * defect[pl.ds(0, 1), :]), unroll=3)
        fvec[...] = jnp.broadcast_to(across(acc) + pushes[pl.ds(top, 1), :], (8, ns))

    local_state()

    def reach(k):
        both = jnp.concatenate([bm[k], weighted_map[k]], axis=0)
        w = mm(both, rst[k], 1, 1)
        rows = pl.ds(pl.multiple_of(k * nu, nu), nu)
        wst[rows, :] = w[:nu]
        gwst[rows, :] = w[nu:]

    def gather_reach():
        pl.loop(0, top, unroll=5)(reach)
        wst[pl.ds(top * nu, nu), :] = bm[top]
        gwst[pl.ds(top * nu, nu), :] = weighted_map[top]
        mmat[...] = mm(wst[...], gwst[...], 0, 0)

    cx_all.wait_recv()

    x_all.wait_recv()
    plane_costate, totals = line_backward(cx, gx, vloc_x)

    down = remote(dy, vy, e_send.at[2], e_recv.at[2], peer("tm_0", LINE - 1))

    @pl.when(y == LINE - 1)
    def _():
        dy[...] = jnp.broadcast_to(plane_costate, (8, ns))
        down.start()

    omega[...] = line_products(gx, sx, px)

    halves = (high, low)
    second = [remote(omega.at[r], om1.at[r], y_send.at[0], y_recv.at[n], peer("tm_0", 1)) for n, r in enumerate(halves)]
    third = remote(omega, om2, y_send.at[0], y_recv.at[2], peer("tm_0", 1))
    passed = [remote(om1.at[r], om1.at[r], y_send.at[1], y_recv.at[n], peer("tm_0", 1)) for n, r in enumerate(halves)]

    def pass_on(n):
        second[n].wait_recv()
        passed[n].start()

    @pl.when(y == 1)
    def _():
        run(second)

    @pl.when(y == 2)
    def _():
        third.start()

    sy[y] = jnp.broadcast_to(totals, (8, ns))
    s_line, s_all = gather_vectors(2, "tm_0", sy)
    run(s_line)
    line_rest(gz, sz, pz)
    line_rest(gx, sx, px)
    tback[...] = mm(sx[x], sz[z])
    t_zero = col_mv(vloc_x[x, pl.ds(0, 1), :], sz[z]) + vloc_z[z, pl.ds(0, 1), :]

    def combine():
        inward = mm(tback[...], mmat[...])
        answer[...] = mm(inward, tback[...], 1, 1)
        constant = row_mv(tback[...], fvec[pl.ds(0, 1), :]) - row_mv(inward, t_zero)
        avec[...] = jnp.broadcast_to(constant, (8, ns))

    @pl.when(y == 0)
    def _():
        gather_reach()
        combine()

    pl.when(y == 1)(gather_reach)

    @pl.when(y == LINE - 1)
    def _():
        vy[...] = jnp.zeros((8, ns), F32)

    @pl.when(y < LINE - 1)
    def _():
        down.wait_recv()

    plane_in = vy[pl.ds(0, 1), :]

    @pl.when((y == 1) | (y == 2))
    def _():
        dy[...] = jnp.broadcast_to(col_mv(plane_in, omega[...]) + plane_costate, (8, ns))
        down.start()

    @pl.when(y > 1)
    def _():
        gather_reach()

    pl.when(y > 0)(combine)

    here = x * LINE + z
    plane_sum[here, pl.ds(0, 1), :] = avec[pl.ds(0, 1), :] - row_mv(answer[...], plane_in)

    def to_plane(buf, rows, n):
        return [
            remote(buf.at[here, rows], buf.at[here, rows], p_send.at[n], p_recv.at[n], in_plane(i, j)) for i, j in offsets
        ]

    sum_rows, own_rows = pl.ds(0, 1), pl.ds(0, 2)
    run(to_plane(plane_sum, sum_rows, 0))
    v = col_mv(plane_in, tback[...]) + t_zero
    f_own = fvec[pl.ds(0, 1), :] - row_mv(mmat[...], v)
    plane_own[here, pl.ds(0, 1), :] = row_mv(sz[z], f_own)
    plane_own[here, pl.ds(1, 1), :] = f_own
    run(to_plane(plane_own, own_rows, 1))
    others = pl.ds(0, LINE * LINE - 1)
    sum_line = remote(plane_sum.at[others, sum_rows], plane_sum.at[others, sum_rows], p_send.at[0], p_recv.at[0], peer("tm_1", 1))
    own_line = remote(plane_own.at[others, own_rows], plane_own.at[others, own_rows], p_send.at[1], p_recv.at[1], peer("tm_1", 1))

    pl.when(y == 2)(lambda: pass_on(0))

    vc = as_column(v)

    def lift(k):
        at = pl.ds(k, 1)
        after[at, :] = after[at, :] + col_apply(vc, rst[k])

    pl.loop(0, top, unroll=5)(lift)
    after[pl.ds(top, 1), :] = v
    before_first = col_apply(vc, phi[...]) + cvec[pl.ds(0, 1), :]

    pl.loop(0, count, unroll=8)(respond)

    pl.when(y == 2)(lambda: pass_on(1))

    def forward(k, carried):
        correction = carried - defect[pl.ds(k, 1), :]
        state_step[pl.ds(k, 1), :] = correction
        return row_mv(am[k], correction) + pushes[pl.ds(k, 1), :]

    lax.fori_loop(0, count, forward, jnp.zeros((1, ns), F32))

    sum_line.wait_recv()
    plane_state = jnp.sum(plane_sum[:, 0:1, :], axis=0)
    fy[y] = jnp.broadcast_to(plane_state, (8, ns))
    ahead = [
        remote(fy.at[y], fy.at[y], f_send.at[by - 1], f_recv.at[by - 1], peer("tm_0", by)) for by in range(1, LINE)
    ]
    for by in range(1, LINE):
        @pl.when(y + by < LINE)
        def _(by=by):
            ahead[by - 1].start()

    own_line.wait_recv()
    tforw[...] = mm(pz[z], px[x])

    def line_state(vector, maps, at):
        entering = jnp.zeros((1, ns), F32)
        found = entering
        for p in range(LINE - 1):
            entering = row_mv(maps[p], entering) + vector(p) if p else vector(p)
            found = jnp.where(at == p + 1, entering, found)
        return found

    in_line = line_state(lambda p: plane_own[x * LINE + p, pl.ds(1, 1), :], gz, z)
    groups = [jnp.sum(plane_own[LINE * p : LINE * p + LINE, 0:1, :], axis=0) for p in range(LINE)]
    in_group = line_state(lambda p: groups[p], gx, x)
    x_zero = row_mv(pz[z], in_group) + in_line

    for by in range(1, LINE):
        @pl.when(y >= by)
        def _(by=by):
            ahead[by - 1].wait_recv()

    @pl.when(y == 0)
    def _():
        entry[...] = jnp.zeros((8, ns), F32)

    def enter(vector):
        entry[...] = jnp.broadcast_to(vector, (8, ns))

    at_plane = lambda p: fy[p, pl.ds(0, 1), :]

    @pl.when(y == 1)
    def _():
        enter(at_plane(0))

    @pl.when(y == 2)
    def _():
        enter(row_mv(om1[...], at_plane(0)) + at_plane(1))

    @pl.when(y == LINE - 1)
    def _():
        third.wait_recv()
        for copy in passed:
            copy.wait_recv()
        enter(row_mv(om2[...], row_mv(om1[...], at_plane(0)) + at_plane(1)) + at_plane(2))

    x_in = row_mv(tforw[...], entry[pl.ds(0, 1), :]) + x_zero
    xc = as_column(x_in)
    out_x, out_m = pl.ds(0, count), pl.ds(count, count)
    packed[pl.ds(0, 1), :] = state_step[pl.ds(0, 1), :] + x_in

    def settle(k):
        at = pl.ds(k, 1)
        packed[at, :] = state_step[at, :] + col_apply(xc, qt[k])

    pl.loop(1, count, unroll=5)(settle)

    def close(k):
        at = pl.ds(k, 1)
        now = packed[at, :]
        sources[at, :] = row_mv(vm[k], now - defect[at, :])
        input_linear[at, :] = row_mv(fm[k], now)

    pl.loop(0, count, unroll=8)(close)
    packed[pl.ds(count + 1, top), :] = sources[pl.ds(1, top), :] + after[pl.ds(0, top), :]
    packed[pl.ds(count, 1), :] = sources[pl.ds(0, 1), :] + before_first
    chosen = active[...].astype(F32)
    step = (1.0 - chosen) * (input_linear[...] + gain[...]) + chosen * (upper[...] - inputs[...])
    packed[pl.ds(2 * count, count), pl.ds(0, nu)] = step
    weighted = lax.dot_general(
        step, iw[...], (((1,), (1,)), ((), ())), precision=PRECISE, preferred_element_type=F32
    )
    packed[pl.ds(2 * count, count), pl.ds(HALF, nu)] = chosen * (grad_input[...] + weighted + pulled[...])

    s_all.wait_recv()
    totals = jnp.sum(sy[:, 0:1, :], axis=0)
    horizon = count * LINE**3
    pick = lambda n: jnp.sum(jnp.where(lane == n, totals, 0.0), axis=1, keepdims=True)
    primal = pick(0) / (pick(3) + floor_share * horizon * ns)
    dual = pick(1) / (pick(4) + floor_share * horizon * (ns + nu))
    complement = pick(2) / (pick(5) + floor_share * horizon * nu)
    lanes = lax.broadcasted_iota(jnp.int32, (8, ns), 1)
    values = jnp.where(lanes == 0, primal, jnp.where(lanes == 1, dual, complement))
    packed[pl.ds(3 * count, 8), :] = jnp.sqrt(values)

    for copy in [to_prev, to_next, z_all, x_all, c_all, cx_all, s_all, sum_line, own_line]:
        copy.wait_send()

    for by in range(1, LINE):
        @pl.when(y + by < LINE)
        def _(by=by):
            ahead[by - 1].wait_send()

    @pl.when((y == 1) | (y == 2))
    def _():
        third.wait_send()

    @pl.when(y == 2)
    def _():
        remote(om1, om1, y_send.at[1], y_recv.at[0], peer("tm_0", 1)).wait_send()

    @pl.when(y > 0)
    def _():
        down.wait_send()


def unpack(packed, state_step, input_step, multiplier_step, bound_step, norms):
    count, nu = input_step.shape
    state_step[...] = packed[pl.ds(0, count), :]
    multiplier_step[...] = packed[pl.ds(count, count), :]
    input_step[...] = packed[pl.ds(2 * count, count), pl.ds(0, nu)]
    bound_step[...] = packed[pl.ds(2 * count, count), pl.ds(HALF, nu)]
    norms[...] = packed[pl.ds(3 * count, 1), pl.ds(0, HALF)][0, :3]


def local(*args):
    states, inputs = args[12], args[13]
    count, ns = states.shape
    nu = inputs.shape[1]
    v = lambda *shape: pltpu.VMEM(shape, F32)
    dma = lambda *shape: pltpu.SemaphoreType.DMA(shape)
    square = v(ns, ns)
    line = v(LINE, ns, ns)
    rows = v(LINE, 8, ns)
    row = v(8, ns)
    wide, narrow = v(count, ns), v(count, nu)
    scratch = [
        v(count, ns, ns), v(count, nu, ns), v(count, ns, ns), v(count, nu, ns), v(count, ns, ns),
        v(count, nu, nu), v(nu, nu), wide, wide, narrow, wide, narrow,
        wide, narrow, wide, narrow, pltpu.VMEM((count, nu), jnp.int32),
        v(count, ns, ns), v(count, ns, ns), v(count // 2, ns, ns), square, v(count, nu, ns), square, v(count * nu, ns), v(count * nu, ns),
        line, line, line, line, line, line, square, square, square, square, square,
        wide, wide, wide, wide, narrow, wide, wide, narrow, narrow, wide, wide,
        row, row, row, rows, rows, v(LINE * LINE, 8, ns), v(LINE * LINE, 8, ns), rows, row, row, row, row, row, square, rows,
        rows, rows, row,
        dma(14), dma(2), dma(2), dma(2, 3), dma(3), dma(3), dma(3), dma(3),
        dma(2), dma(2), dma(2), dma(3), dma(LINE - 1), dma(LINE - 1),
    ]
    vmem = pl.BlockSpec(memory_space=pltpu.VMEM)
    packed = pl.pallas_call(
        kernel,
        out_shape=pltpu.VMEM((3 * count + 8, ns), F32),
        in_specs=[pl.BlockSpec(memory_space=pl.ANY)] * len(args),
        out_specs=vmem,
        scratch_shapes=scratch,
        compiler_params=pltpu.CompilerParams(
            collective_id=0, has_side_effects=True, vmem_limit_bytes=56 * 1024 * 1024
        ),
        name="riccati",
    )(*args)
    return pl.pallas_call(
        unpack,
        out_shape=[
            jax.ShapeDtypeStruct((count, ns), F32),
            jax.ShapeDtypeStruct((count, nu), F32),
            jax.ShapeDtypeStruct((count, ns), F32),
            jax.ShapeDtypeStruct((count, nu), F32),
            jax.ShapeDtypeStruct((3,), F32),
        ],
        in_specs=[vmem],
        out_specs=[vmem] * 5,
        name="unpack",
    )(pltpu.with_memory_space_constraint(packed, pltpu.VMEM))


def solution(mesh):
    lines = Mesh(
        mesh.devices.reshape(LINE, LINE, LINE, mesh.shape["batch"]), ("tm_0", "tm_1", "tm_2", "batch")
    )
    cube, flat = P(BATCH_TM, None, None), P(BATCH_TM, None)
    return jax.shard_map(
        local,
        mesh=lines,
        in_specs=(cube,) * 6 + (P("batch", None),) + (flat,) * 10,
        out_specs=(flat, flat, flat, flat, P("batch")),
        check_vma=False,
    )
```

```python
import jax
import jax.numpy as jnp
from jax import lax
from jax.experimental import pallas as pl
from jax.experimental.pallas import tpu as pltpu
from jax.sharding import Mesh
from jax.sharding import PartitionSpec as P

TM = ("tm_0", "tm_1", "tm_2")
BATCH_TM = ("batch", "tm_0", "tm_1", "tm_2")
MESH = pl.DeviceIdType.MESH
F32 = jnp.float32
BF16 = jnp.bfloat16
PRECISE = lax.Precision.HIGHEST
floor_share = 0.001
LINE = 4
HALF = 128


def split(a):
    high = a.astype(BF16)
    return high, (a - high.astype(F32)).astype(BF16)


def mm(a, b, ca=1, cb=0):
    dims = (((ca,), (cb,)), ((), ()))
    ah, al = split(a)
    bh, bl = split(b)
    dot = lambda x, y: lax.dot_general(x, y, dims, preferred_element_type=F32)
    return dot(ah, bh) + dot(ah, bl) + dot(al, bh)


def fold(t):
    return t[:, :HALF] + t[:, HALF:] if t.shape[1] > HALF else t


def across(t):
    return jnp.sum(jnp.transpose(t), axis=0, keepdims=True)


def row_mv(w, x):
    return across(fold(w * x))


def as_column(v):
    return jnp.transpose(jnp.broadcast_to(v, (HALF, v.shape[1])))


def col_apply(vc, w):
    n = w.shape[1]
    if n > HALF:
        vc = jnp.concatenate([vc] * (n // HALF), axis=1)
    else:
        vc = vc[:, :n]
    return jnp.sum(vc * w, axis=0, keepdims=True)


def col_mv(v, w):
    return col_apply(as_column(v), w)


def identity_matrix(n):
    i = lax.broadcasted_iota(jnp.int32, (n, n), 0)
    j = lax.broadcasted_iota(jnp.int32, (n, n), 1)
    return jnp.where(i == j, 1.0, 0.0).astype(F32)


def line_products(maps, suffix, prefix):
    n = maps.shape[1]
    upper = mm(maps[3], maps[2])
    lower = mm(maps[1], maps[0])
    suffix[1] = upper
    prefix[2] = lower
    return mm(upper, lower)


def line_rest(maps, suffix, prefix):
    eye = identity_matrix(maps.shape[1])
    suffix[3] = eye
    prefix[0] = eye
    suffix[2] = maps[3]
    prefix[1] = maps[0]
    suffix[0] = mm(suffix[1], maps[1])
    prefix[3] = mm(maps[2], prefix[2])


def kernel(
    state_map_h, input_map_h, closed_loop_h, feedback_h, value_h, gain_h, weight_h,
    state_weight_h, state_linear_h, input_linear_h, offset_h, upper_h, states_h, inputs_h,
    multipliers_h, bound_h, active_h,
    packed,
    sm, bm, am, fm, vm, gm, iw, state_weight, state_linear, input_linear, offset, upper,
    states, inputs, mult, bound, active,
    rst, qt, tree, phi, weighted_map, mmat, wst, gwst,
    gz, gx, sz, pz, sx, px, omega, om1, om2, tback, tforw,
    predicted, following, defect, grad_state, grad_input, sources, after, pulled, gain, pushes, state_step,
    edge, from_next, from_prev, cz, cx, plane_sum, plane_own, fy, vy, dy, entry, fvec, avec, answer, sy,
    vloc_z, vloc_x, cvec,
    in_sem, a_sem, m_send, m_recv, v_send, v_recv, e_send, e_recv, p_send, p_recv, y_send, y_recv, f_send, f_recv,
):
    count, ns = states.shape
    nu = inputs.shape[1]
    y, x, z = (lax.axis_index(a) for a in TM)
    core = lax.axis_index("batch")
    place = (y * LINE + x) * LINE + z
    last = LINE**3 - 1
    top = count - 1

    def device_at(index):
        return {
            "tm_0": lax.div(index, LINE * LINE),
            "tm_1": lax.rem(lax.div(index, LINE), LINE),
            "tm_2": lax.rem(index, LINE),
        }

    next_device = device_at(lax.rem(place + 1, last + 1))
    prev_device = device_at(lax.rem(place + last, last + 1))
    has_next, has_prev = pl.when(place < last), pl.when(place > 0)
    spot = {"tm_0": y, "tm_1": x, "tm_2": z}

    def peer(axis, by):
        return {axis: lax.rem(spot[axis] + by, LINE)}

    offsets = [(i, j) for i in range(LINE) for j in range(LINE) if i or j]

    def in_plane(i, j):
        return {"tm_1": lax.rem(x + i, LINE), "tm_2": lax.rem(z + j, LINE)}

    first_half, last_half = pl.ds(0, count // 2), pl.ds(count // 2, count // 2)
    a_copies = [
        pltpu.make_async_copy(closed_loop_h.at[k], am.at[k], a_sem.at[k // (count // 2)]) for k in range(count)
    ]
    a_halves = [
        pltpu.make_async_copy(closed_loop_h.at[part], am.at[part], a_sem.at[n])
        for n, part in enumerate((first_half, last_half))
    ]
    pairs = [
        (states_h, states), (inputs_h, inputs), (input_map_h.at[top], bm.at[top]), (state_map_h.at[top], sm.at[top]),
        (multipliers_h, mult), (input_map_h.at[pl.ds(0, top)], bm.at[pl.ds(0, top)]),
        (state_map_h.at[pl.ds(0, 8)], sm.at[pl.ds(0, 8)]),
        (state_map_h.at[pl.ds(8, top - 8)], sm.at[pl.ds(8, top - 8)]), (state_weight_h, state_weight),
        (state_linear_h, state_linear), (input_linear_h, input_linear), (offset_h, offset), (upper_h, upper),
        (bound_h, bound), (active_h, active), (weight_h, iw), (value_h, vm), (feedback_h, fm), (gain_h, gm),
    ]
    in_copies = [pltpu.make_async_copy(s, d, in_sem.at[n if n < 14 else n - 14]) for n, (s, d) in enumerate(pairs)]
    for copy in in_copies[:5]:
        copy.start()
    for copy in a_copies:
        copy.start()

    barrier = pltpu.get_barrier_semaphore()
    for by in range(1, LINE):
        pl.semaphore_signal(barrier, inc=1, device_id=peer("tm_0", by), device_id_type=MESH)
    for i, j in offsets:
        pl.semaphore_signal(barrier, inc=1, device_id=in_plane(i, j), device_id_type=MESH)
    has_next(lambda: pl.semaphore_signal(barrier, inc=1, device_id=next_device, device_id_type=MESH))
    has_prev(lambda: pl.semaphore_signal(barrier, inc=1, device_id=prev_device, device_id_type=MESH))

    def predict(k):
        at = pl.ds(k, 1)
        predicted[at, :] = row_mv(sm[k], states[at, :]) + col_mv(inputs[at, :], bm[k])

    a_halves[0].wait()
    for i in range(count // 4):
        tree[i] = mm(am[2 * i + 1], am[2 * i])
    for copy in a_halves[1:] + in_copies[:5]:
        copy.wait()
    predict(top)
    edge[...] = jnp.broadcast_to(predicted[pl.ds(top, 1), :], (8, ns))
    for copy in in_copies[5:]:
        copy.start()
    for i in range(count // 4, count // 2):
        tree[i] = mm(am[2 * i + 1], am[2 * i])
    level = [tree[i] for i in range(count // 2)]
    while len(level) > 1:
        level = [mm(level[i + 1], level[i]) for i in range(0, len(level), 2)]
    phi[...] = level[0]
    gz[z] = level[0]

    ends = lax.div(place + last, last + 1) + lax.div(2 * last - place, last + 1)
    pl.semaphore_wait(barrier, (LINE - 1) + len(offsets) + ends)

    def remote(src, dst, send, recv, device):
        return pltpu.make_async_remote_copy(
            src_ref=src, dst_ref=dst, send_sem=send, recv_sem=recv, device_id=device, device_id_type=MESH
        )

    part = ns // 4
    high, low = pl.ds(0, 2 * part), pl.ds(2 * part, 2 * part)
    quarters = [pl.ds(n * part, part) for n in range(4)]

    def gather_maps(stage, axis, maps):
        at = spot[axis]
        right, left = peer(axis, 1), peer(axis, LINE - 1)
        before, behind = lax.rem(at + LINE - 1, LINE), lax.rem(at + 1, LINE)
        plan = [
            (at, quarters[0], right), (at, quarters[3], left), (at, quarters[1], right), (at, quarters[2], left),
            (at, low, right), (at, high, left),
            (before, quarters[0], right), (behind, quarters[3], left),
            (before, quarters[1], right), (behind, quarters[2], left),
        ]
        sems = (0, 0, 1, 1, 2, 2, 2, 2, 2, 2)
        copies = [
            remote(maps.at[s, rows], maps.at[s, rows], m_send.at[stage], m_recv.at[stage, n], dev)
            for n, (s, rows, dev) in zip(sems, plan)
        ]
        whole = remote(maps.at[pl.ds(0, 3)], maps.at[pl.ds(0, 2)], m_send.at[stage], m_recv.at[stage, 2], right)
        return copies, whole

    def relay(copies, maps, stage, turn):
        remote(maps.at[0, high], maps.at[0, high], m_send.at[stage], m_recv.at[stage, turn], peer("tm_0", 1)).wait_recv()
        run(copies[2 * turn + 6 : 2 * turn + 8])

    def gather_vectors(stage, axis, buf):
        at = spot[axis]
        copies = [
            remote(buf.at[at], buf.at[at], v_send.at[stage], v_recv.at[stage], peer(axis, by)) for by in range(1, LINE)
        ]
        three = buf.at[pl.ds(0, LINE - 1)]
        return copies, remote(three, three, v_send.at[stage], v_recv.at[stage], peer(axis, 1))

    def run(copies):
        for copy in copies:
            copy.start()

    to_prev = remote(mult.at[pl.ds(0, 8)], from_next, e_send.at[0], e_recv.at[0], prev_device)
    to_next = remote(edge, from_prev, e_send.at[1], e_recv.at[1], next_device)
    z_maps, z_all = gather_maps(0, "tm_2", gz)
    has_prev(to_prev.start)
    has_next(to_next.start)
    half = count // 2

    @pl.when(core == 0)
    def _():
        run(z_maps[:6])

    qt[1] = jnp.transpose(am[0])
    qt[2] = jnp.transpose(tree[0])

    def prefix_step(i):
        prefix = qt[2 * i]
        qt[2 * i + 1] = mm(prefix, am[2 * i], 1, 1)
        qt[2 * i + 2] = mm(prefix, tree[i], 1, 1)

    pl.loop(1, half - 1)(prefix_step)
    qt[top] = mm(qt[top - 1], am[top - 1], 1, 1)

    @pl.when(core == 0)
    def _():
        relay(z_maps, gz, 0, 0)

    for copy in in_copies[5:8]:
        copy.wait()
    pl.loop(0, top, unroll=5)(predict)

    @pl.when(core == 0)
    def _():
        relay(z_maps, gz, 0, 1)

    for copy in in_copies[8:16]:
        copy.wait()
    has_next(to_prev.wait_recv)

    @pl.when(place == last)
    def _():
        from_next[...] = jnp.zeros((8, ns), F32)

    following[pl.ds(0, top), :] = mult[pl.ds(1, top), :]
    following[pl.ds(top, 1), :] = from_next[pl.ds(0, 1), :]

    def gradients(k):
        at = pl.ds(k, 1)
        ahead = following[at, :]
        grad_state[at, :] = col_mv(ahead, sm[k])
        grad_input[at, :] = row_mv(bm[k], ahead)

    pl.loop(0, count, unroll=4)(gradients)
    grad_state[...] = state_weight[...] * states[...] + state_linear[...] + mult[...] - grad_state[...]
    weighted = lax.dot_general(
        inputs[...], iw[...], (((1,), (1,)), ((), ())), precision=PRECISE, preferred_element_type=F32
    )
    grad_input[...] = weighted + input_linear[...] - grad_input[...] + bound[...]

    def suffix_step(i):
        j = half - 1 - i
        suffix = rst[2 * j + 1]
        rst[2 * j] = mm(suffix, am[2 * j + 1])
        rst[2 * j - 1] = mm(suffix, tree[j])

    def suffixes():
        rst[top - 1] = am[top]
        rst[top - 2] = tree[half - 1]
        pl.loop(1, half - 1)(suffix_step)
        rst[0] = mm(rst[1], am[1])

    for copy in in_copies[16:]:
        copy.wait()
    has_prev(to_next.wait_recv)

    @pl.when(place == 0)
    def _():
        from_prev[...] = jnp.zeros((8, ns), F32)

    defect[pl.ds(1, top), :] = states[pl.ds(1, top), :] - predicted[pl.ds(0, top), :] - offset[pl.ds(1, top), :]
    entered = from_prev[pl.ds(0, 1), :]
    defect[pl.ds(0, 1), :] = states[pl.ds(0, 1), :] - entered - offset[pl.ds(0, 1), :]

    def source(k):
        at = pl.ds(k, 1)
        sources[at, :] = row_mv(vm[k], defect[at, :]) + grad_state[at, :] + col_mv(grad_input[at, :], fm[k])
        weighted_map[k] = mm(gm[k], bm[k])

    pl.loop(0, count, unroll=4)(source)

    @pl.when(core == 1)
    def _():
        run(z_maps[:6])
        suffixes()

    @pl.when(core == 1)
    def _():
        relay(z_maps, gz, 0, 0)
        relay(z_maps, gz, 0, 1)


    def gather_source(k, acc):
        return acc + fold(qt[k] * sources[pl.ds(k, 1), :])

    acc = lax.fori_loop(1, count, gather_source, jnp.zeros((ns, HALF), F32), unroll=3)
    local_costate = across(acc) + sources[pl.ds(0, 1), :]
    cvec[pl.ds(0, 1), :] = local_costate

    slack = bound[...] * (upper[...] - inputs[...])
    lane = lax.broadcasted_iota(jnp.int32, (1, ns), 1)
    squares = lambda t: jnp.sum(t * t)
    sums = [
        squares(defect[...]), squares(grad_state[...]) + squares(grad_input[...]), squares(slack),
        squares(offset[...]), squares(state_linear[...]) + squares(input_linear[...]), squares(bound[...]),
    ]
    stats = jnp.zeros((1, ns), F32)
    for n, s in enumerate(sums):
        stats = jnp.where(lane == n, s, stats)

    cz[z, pl.ds(0, 1), :] = local_costate
    cz[z, pl.ds(1, 1), :] = stats
    cz[z, pl.ds(2, 6), :] = jnp.zeros((6, ns), F32)
    c_line, c_all = gather_vectors(0, "tm_2", cz)
    run(c_line)

    def reach(k):
        both = jnp.concatenate([bm[k], weighted_map[k]], axis=0)
        w = mm(both, rst[k], 1, 1)
        rows = pl.ds(pl.multiple_of(k * nu, nu), nu)
        wst[rows, :] = w[:nu]
        gwst[rows, :] = w[nu:]

    def reach_all():
        pl.loop(0, top, unroll=5)(reach)
        wst[pl.ds(top * nu, nu), :] = bm[top]
        gwst[pl.ds(top * nu, nu), :] = weighted_map[top]

    pl.when(core == 1)(reach_all)

    z_all.wait_recv()
    gx[x] = line_products(gz, sz, pz)
    x_maps, x_all = gather_maps(1, "tm_1", gx)

    def line_backward(buf, maps, store):
        v = buf[LINE - 1, pl.ds(0, 1), :]
        store[LINE - 1] = jnp.zeros((8, ns), F32)
        for p in reversed(range(LINE - 1)):
            store[p] = jnp.broadcast_to(v, (8, ns))
            v = col_mv(v, maps[p]) + buf[p, pl.ds(0, 1), :]
        total = jnp.sum(buf[:, 1:2, :], axis=0)
        return v, total

    run(x_maps[:6])

    pl.when(core == 0)(suffixes)

    c_all.wait_recv()
    group_costate, totals = line_backward(cz, gz, vloc_z)
    cx[x, pl.ds(0, 1), :] = group_costate
    cx[x, pl.ds(1, 1), :] = totals
    cx[x, pl.ds(2, 6), :] = jnp.zeros((6, ns), F32)
    cx_line, cx_all = gather_vectors(1, "tm_1", cx)
    run(cx_line)

    pl.when(core == 0)(lambda: relay(x_maps, gx, 1, 0))

    def backward(i, v):
        k = top - i
        after[pl.ds(k, 1), :] = v
        return col_mv(v, am[k]) + sources[pl.ds(k, 1), :]

    v = lax.fori_loop(0, half // 2, backward, jnp.zeros((1, ns), F32))
    pl.when(core == 0)(lambda: relay(x_maps, gx, 1, 1))
    lax.fori_loop(half // 2, count, backward, v)

    @pl.when(core == 1)
    def _():
        relay(x_maps, gx, 1, 0)
        relay(x_maps, gx, 1, 1)

    def respond(k):
        at = pl.ds(k, 1)
        pull = row_mv(bm[k], after[at, :])
        pulled[at, :] = pull
        step = -row_mv(gm[k], grad_input[at, :] + pull)
        gain[at, :] = step
        pushes[at, :] = col_mv(step, bm[k])

    def gather_push(k, acc):
        return acc + fold(rst[k] * (pushes[pl.ds(k, 1), :] - defect[pl.ds(k + 1, 1), :]))

    def local_state():
        pl.loop(0, count, unroll=8)(respond)
        acc = lax.fori_loop(0, top, gather_push, -fold(phi[...] * defect[pl.ds(0, 1), :]), unroll=3)
        fvec[...] = jnp.broadcast_to(across(acc) + pushes[pl.ds(top, 1), :], (8, ns))

    local_state()

    def gather_reach():
        pl.when(core == 0)(reach_all)
        mmat[...] = mm(wst[...], gwst[...], 0, 0)

    line_rest(gz, sz, pz)
    cx_all.wait_recv()

    x_all.wait_recv()
    plane_costate, totals = line_backward(cx, gx, vloc_x)

    down = remote(dy, vy, e_send.at[2], e_recv.at[2], peer("tm_0", LINE - 1))

    @pl.when(y == LINE - 1)
    def _():
        dy[...] = jnp.broadcast_to(plane_costate, (8, ns))
        down.start()

    omega[...] = line_products(gx, sx, px)

    halves = (high, low)
    second = [remote(omega.at[r], om1.at[r], y_send.at[0], y_recv.at[n], peer("tm_0", 1)) for n, r in enumerate(halves)]
    third = remote(omega, om2, y_send.at[0], y_recv.at[2], peer("tm_0", 1))
    passed = [remote(om1.at[r], om1.at[r], y_send.at[1], y_recv.at[n], peer("tm_0", 1)) for n, r in enumerate(halves)]

    def pass_on(n):
        second[n].wait_recv()
        passed[n].start()

    @pl.when(y == 1)
    def _():
        run(second)

    @pl.when(y == 2)
    def _():
        third.start()

    sy[y] = jnp.broadcast_to(totals, (8, ns))
    s_line, s_all = gather_vectors(2, "tm_0", sy)
    run(s_line)
    line_rest(gx, sx, px)
    tback[...] = mm(sx[x], sz[z])
    t_zero = col_mv(vloc_x[x, pl.ds(0, 1), :], sz[z]) + vloc_z[z, pl.ds(0, 1), :]

    def combine():
        inward = mm(tback[...], mmat[...])
        answer[...] = mm(inward, tback[...], 1, 1)
        constant = row_mv(tback[...], fvec[pl.ds(0, 1), :]) - row_mv(inward, t_zero)
        avec[...] = jnp.broadcast_to(constant, (8, ns))

    @pl.when(y == 0)
    def _():
        gather_reach()
        combine()

    pl.when(y == 1)(gather_reach)

    @pl.when(y == LINE - 1)
    def _():
        vy[...] = jnp.zeros((8, ns), F32)

    @pl.when(y < LINE - 1)
    def _():
        down.wait_recv()

    plane_in = vy[pl.ds(0, 1), :]

    @pl.when((y == 1) | (y == 2))
    def _():
        dy[...] = jnp.broadcast_to(col_mv(plane_in, omega[...]) + plane_costate, (8, ns))
        down.start()

    @pl.when(y > 1)
    def _():
        gather_reach()

    pl.when(y > 0)(combine)

    here = x * LINE + z
    plane_sum[here, pl.ds(0, 1), :] = avec[pl.ds(0, 1), :] - row_mv(answer[...], plane_in)

    def to_plane(buf, rows, n):
        return [
            remote(buf.at[here, rows], buf.at[here, rows], p_send.at[n], p_recv.at[n], in_plane(i, j)) for i, j in offsets
        ]

    sum_rows, own_rows = pl.ds(0, 1), pl.ds(0, 2)
    run(to_plane(plane_sum, sum_rows, 0))
    v = col_mv(plane_in, tback[...]) + t_zero
    f_own = fvec[pl.ds(0, 1), :] - row_mv(mmat[...], v)
    plane_own[here, pl.ds(0, 1), :] = row_mv(sz[z], f_own)
    plane_own[here, pl.ds(1, 1), :] = f_own
    run(to_plane(plane_own, own_rows, 1))
    others = pl.ds(0, LINE * LINE - 1)
    sum_line = remote(plane_sum.at[others, sum_rows], plane_sum.at[others, sum_rows], p_send.at[0], p_recv.at[0], peer("tm_1", 1))
    own_line = remote(plane_own.at[others, own_rows], plane_own.at[others, own_rows], p_send.at[1], p_recv.at[1], peer("tm_1", 1))

    pl.when(y == 2)(lambda: pass_on(0))

    vc = as_column(v)

    def lift(k):
        at = pl.ds(k, 1)
        after[at, :] = after[at, :] + col_apply(vc, rst[k])

    pl.loop(0, top, unroll=5)(lift)
    after[pl.ds(top, 1), :] = v
    before_first = col_apply(vc, phi[...]) + cvec[pl.ds(0, 1), :]

    pl.loop(0, count, unroll=8)(respond)

    pl.when(y == 2)(lambda: pass_on(1))

    def forward(k, carried):
        correction = carried - defect[pl.ds(k, 1), :]
        state_step[pl.ds(k, 1), :] = correction
        return row_mv(am[k], correction) + pushes[pl.ds(k, 1), :]

    def local_steps():
        lax.fori_loop(0, count, forward, jnp.zeros((1, ns), F32))

    local_steps()

    sum_line.wait_recv()
    plane_state = jnp.sum(plane_sum[:, 0:1, :], axis=0)
    fy[y] = jnp.broadcast_to(plane_state, (8, ns))
    ahead = [
        remote(fy.at[y], fy.at[y], f_send.at[by - 1], f_recv.at[by - 1], peer("tm_0", by)) for by in range(1, LINE)
    ]
    for by in range(1, LINE):
        @pl.when(y + by < LINE)
        def _(by=by):
            ahead[by - 1].start()

    own_line.wait_recv()
    tforw[...] = mm(pz[z], px[x])

    def line_state(vector, maps, at):
        entering = jnp.zeros((1, ns), F32)
        found = entering
        for p in range(LINE - 1):
            entering = row_mv(maps[p], entering) + vector(p) if p else vector(p)
            found = jnp.where(at == p + 1, entering, found)
        return found

    in_line = line_state(lambda p: plane_own[x * LINE + p, pl.ds(1, 1), :], gz, z)
    groups = [jnp.sum(plane_own[LINE * p : LINE * p + LINE, 0:1, :], axis=0) for p in range(LINE)]
    in_group = line_state(lambda p: groups[p], gx, x)
    x_zero = row_mv(pz[z], in_group) + in_line

    at_plane = lambda p: fy[p, pl.ds(0, 1), :]

    def set_base(vector):
        avec[...] = jnp.broadcast_to(vector, (8, ns))

    @pl.when(y <= 1)
    def _():
        set_base(x_zero)

    @pl.when(y == 2)
    def _():
        through = tforw[...]
        tforw[...] = mm(through, om1[...])
        ahead[0].wait_recv()
        set_base(row_mv(through, at_plane(1)) + x_zero)

    @pl.when(y == LINE - 1)
    def _():
        through = tforw[...]
        third.wait_recv()
        for copy in passed:
            copy.wait_recv()
        tforw[...] = mm(mm(through, om2[...]), om1[...])
        ahead[0].wait_recv()
        ahead[1].wait_recv()
        set_base(row_mv(through, row_mv(om2[...], at_plane(1)) + at_plane(2)) + x_zero)

    @pl.when(y == 0)
    def _():
        entry[...] = avec[...]

    for by in range(1, LINE):
        @pl.when(y == by)
        def _(by=by):
            ahead[by - 1].wait_recv()
            entry[...] = jnp.broadcast_to(row_mv(tforw[...], at_plane(0)), (8, ns)) + avec[...]

    x_in = entry[pl.ds(0, 1), :]
    xc = as_column(x_in)
    out_x, out_m = pl.ds(0, count), pl.ds(count, count)
    packed[pl.ds(0, 1), :] = state_step[pl.ds(0, 1), :] + x_in

    def settle(k):
        at = pl.ds(k, 1)
        packed[at, :] = state_step[at, :] + col_apply(xc, qt[k])

    pl.loop(1, count, unroll=5)(settle)

    def close(k):
        at = pl.ds(k, 1)
        now = packed[at, :]
        sources[at, :] = row_mv(vm[k], now - defect[at, :])
        input_linear[at, :] = row_mv(fm[k], now)

    pl.loop(0, count, unroll=8)(close)
    packed[pl.ds(count + 1, top), :] = sources[pl.ds(1, top), :] + after[pl.ds(0, top), :]
    packed[pl.ds(count, 1), :] = sources[pl.ds(0, 1), :] + before_first
    chosen = active[...].astype(F32)
    step = (1.0 - chosen) * (input_linear[...] + gain[...]) + chosen * (upper[...] - inputs[...])
    packed[pl.ds(2 * count, count), pl.ds(0, nu)] = step
    weighted = lax.dot_general(
        step, iw[...], (((1,), (1,)), ((), ())), precision=PRECISE, preferred_element_type=F32
    )
    packed[pl.ds(2 * count, count), pl.ds(HALF, nu)] = chosen * (grad_input[...] + weighted + pulled[...])

    s_all.wait_recv()
    totals = jnp.sum(sy[:, 0:1, :], axis=0)
    horizon = count * LINE**3
    pick = lambda n: jnp.sum(jnp.where(lane == n, totals, 0.0), axis=1, keepdims=True)
    primal = pick(0) / (pick(3) + floor_share * horizon * ns)
    dual = pick(1) / (pick(4) + floor_share * horizon * (ns + nu))
    complement = pick(2) / (pick(5) + floor_share * horizon * nu)
    lanes = lax.broadcasted_iota(jnp.int32, (8, ns), 1)
    values = jnp.where(lanes == 0, primal, jnp.where(lanes == 1, dual, complement))
    packed[pl.ds(3 * count, 8), :] = jnp.sqrt(values)

    has_prev(to_prev.wait_send)
    has_next(to_next.wait_send)
    for copy in [z_all, x_all, c_all, cx_all, s_all, sum_line, own_line]:
        copy.wait_send()

    for by in range(1, LINE):
        @pl.when(y + by < LINE)
        def _(by=by):
            ahead[by - 1].wait_send()

    @pl.when((y == 1) | (y == 2))
    def _():
        third.wait_send()

    @pl.when(y == 2)
    def _():
        remote(om1, om1, y_send.at[1], y_recv.at[0], peer("tm_0", 1)).wait_send()

    @pl.when(y > 0)
    def _():
        down.wait_send()


def unpack(packed, state_step, input_step, multiplier_step, bound_step, norms):
    count, nu = input_step.shape
    state_step[...] = packed[pl.ds(0, count), :]
    multiplier_step[...] = packed[pl.ds(count, count), :]
    input_step[...] = packed[pl.ds(2 * count, count), pl.ds(0, nu)]
    bound_step[...] = packed[pl.ds(2 * count, count), pl.ds(HALF, nu)]
    norms[...] = packed[pl.ds(3 * count, 1), pl.ds(0, HALF)][0, :3]


def local(*args):
    states, inputs = args[12], args[13]
    count, ns = states.shape
    nu = inputs.shape[1]
    v = lambda *shape: pltpu.VMEM(shape, F32)
    dma = lambda *shape: pltpu.SemaphoreType.DMA(shape)
    square = v(ns, ns)
    line = v(LINE, ns, ns)
    rows = v(LINE, 8, ns)
    row = v(8, ns)
    wide, narrow = v(count, ns), v(count, nu)
    scratch = [
        v(count, ns, ns), v(count, nu, ns), v(count, ns, ns), v(count, nu, ns), v(count, ns, ns),
        v(count, nu, nu), v(nu, nu), wide, wide, narrow, wide, narrow,
        wide, narrow, wide, narrow, pltpu.VMEM((count, nu), jnp.int32),
        v(count, ns, ns), v(count, ns, ns), v(count // 2, ns, ns), square, v(count, nu, ns), square, v(count * nu, ns), v(count * nu, ns),
        line, line, line, line, line, line, square, square, square, square, square,
        wide, wide, wide, wide, narrow, wide, wide, narrow, narrow, wide, wide,
        row, row, row, rows, rows, v(LINE * LINE, 8, ns), v(LINE * LINE, 8, ns), rows, row, row, row, row, row, square, rows,
        rows, rows, row,
        dma(14), dma(2), dma(2), dma(2, 3), dma(3), dma(3), dma(3), dma(3),
        dma(2), dma(2), dma(2), dma(3), dma(LINE - 1), dma(LINE - 1),
    ]
    vmem = pl.BlockSpec(memory_space=pltpu.VMEM)
    packed = pl.pallas_call(
        kernel,
        out_shape=pltpu.VMEM((3 * count + 8, ns), F32),
        in_specs=[pl.BlockSpec(memory_space=pl.ANY)] * len(args),
        out_specs=vmem,
        scratch_shapes=scratch,
        compiler_params=pltpu.CompilerParams(
            collective_id=0, has_side_effects=True, vmem_limit_bytes=56 * 1024 * 1024
        ),
        name="riccati",
    )(*args)
    return pl.pallas_call(
        unpack,
        out_shape=[
            jax.ShapeDtypeStruct((count, ns), F32),
            jax.ShapeDtypeStruct((count, nu), F32),
            jax.ShapeDtypeStruct((count, ns), F32),
            jax.ShapeDtypeStruct((count, nu), F32),
            jax.ShapeDtypeStruct((3,), F32),
        ],
        in_specs=[vmem],
        out_specs=[vmem] * 5,
        name="unpack",
    )(pltpu.with_memory_space_constraint(packed, pltpu.VMEM))


def solution(mesh):
    lines = Mesh(
        mesh.devices.reshape(LINE, LINE, LINE, mesh.shape["batch"]), ("tm_0", "tm_1", "tm_2", "batch")
    )
    cube, flat = P(BATCH_TM, None, None), P(BATCH_TM, None)
    return jax.shard_map(
        local,
        mesh=lines,
        in_specs=(cube,) * 6 + (P("batch", None),) + (flat,) * 10,
        out_specs=(flat, flat, flat, flat, P("batch")),
        check_vma=False,
    )
```

```python
import jax
import jax.numpy as jnp
from jax import lax
from jax.experimental import pallas as pl
from jax.experimental.pallas import tpu as pltpu
from jax.sharding import Mesh
from jax.sharding import PartitionSpec as P

TM = ("tm_0", "tm_1", "tm_2")
BATCH_TM = ("batch", "tm_0", "tm_1", "tm_2")
MESH = pl.DeviceIdType.MESH
F32 = jnp.float32
BF16 = jnp.bfloat16
PRECISE = lax.Precision.HIGHEST
floor_share = 0.001
LINE = 4
HALF = 128


def split(a):
    high = a.astype(BF16)
    return high, (a - high.astype(F32)).astype(BF16)


def mm(a, b, ca=1, cb=0):
    dims = (((ca,), (cb,)), ((), ()))
    ah, al = split(a)
    bh, bl = split(b)
    dot = lambda x, y: lax.dot_general(x, y, dims, preferred_element_type=F32)
    return dot(ah, bh) + dot(ah, bl) + dot(al, bh)


def fold(t):
    return t[:, :HALF] + t[:, HALF:] if t.shape[1] > HALF else t


def across(t):
    return jnp.sum(jnp.transpose(t), axis=0, keepdims=True)


def row_mv(w, x):
    return across(fold(w * x))


def as_column(v):
    return jnp.transpose(jnp.broadcast_to(v, (HALF, v.shape[1])))


def col_apply(vc, w):
    n = w.shape[1]
    if n > HALF:
        vc = jnp.concatenate([vc] * (n // HALF), axis=1)
    else:
        vc = vc[:, :n]
    return jnp.sum(vc * w, axis=0, keepdims=True)


def col_mv(v, w):
    return col_apply(as_column(v), w)


def identity_matrix(n):
    i = lax.broadcasted_iota(jnp.int32, (n, n), 0)
    j = lax.broadcasted_iota(jnp.int32, (n, n), 1)
    return jnp.where(i == j, 1.0, 0.0).astype(F32)


def line_products(maps, suffix, prefix):
    n = maps.shape[1]
    upper = mm(maps[3], maps[2])
    lower = mm(maps[1], maps[0])
    suffix[1] = upper
    prefix[2] = lower
    return mm(upper, lower)


def line_rest(maps, suffix, prefix):
    eye = identity_matrix(maps.shape[1])
    suffix[3] = eye
    prefix[0] = eye
    suffix[2] = maps[3]
    prefix[1] = maps[0]
    suffix[0] = mm(suffix[1], maps[1])
    prefix[3] = mm(maps[2], prefix[2])


def kernel(
    state_map_h, input_map_h, closed_loop_h, feedback_h, value_h, gain_h, weight_h,
    state_weight_h, state_linear_h, input_linear_h, offset_h, upper_h, states_h, inputs_h,
    multipliers_h, bound_h, active_h,
    packed,
    sm, bm, am, fm, vm, gm, iw, state_weight, state_linear, input_linear, offset, upper,
    states, inputs, mult, bound, active,
    rst, qt, tree, phi, weighted_map, mmat, wst, gwst,
    gz, gx, sz, pz, sx, px, omega, om1, om2, tback, tforw,
    predicted, following, defect, grad_state, grad_input, sources, after, pulled, gain, pushes, state_step,
    edge, from_next, from_prev, cz, cx, plane_sum, plane_own, fy, vy, dy, entry, fvec, avec, answer, sy,
    vloc_z, vloc_x, cvec,
    in_sem, a_sem, m_send, m_recv, v_send, v_recv, e_send, e_recv, p_send, p_recv, y_send, y_recv, f_send, f_recv,
):
    count, ns = states.shape
    nu = inputs.shape[1]
    y, x, z = (lax.axis_index(a) for a in TM)
    core = lax.axis_index("batch")
    place = (y * LINE + x) * LINE + z
    last = LINE**3 - 1
    top = count - 1

    def device_at(index):
        return {
            "tm_0": lax.div(index, LINE * LINE),
            "tm_1": lax.rem(lax.div(index, LINE), LINE),
            "tm_2": lax.rem(index, LINE),
        }

    next_device = device_at(lax.rem(place + 1, last + 1))
    prev_device = device_at(lax.rem(place + last, last + 1))
    has_next, has_prev = pl.when(place < last), pl.when(place > 0)
    spot = {"tm_0": y, "tm_1": x, "tm_2": z}

    def peer(axis, by):
        return {axis: lax.rem(spot[axis] + by, LINE)}

    offsets = [(i, j) for i in range(LINE) for j in range(LINE) if i or j]

    def in_plane(i, j):
        return {"tm_1": lax.rem(x + i, LINE), "tm_2": lax.rem(z + j, LINE)}

    first_half, last_half = pl.ds(0, count // 2), pl.ds(count // 2, count // 2)
    a_copies = [
        pltpu.make_async_copy(closed_loop_h.at[k], am.at[k], a_sem.at[k // (count // 2)]) for k in range(count)
    ]
    a_halves = [
        pltpu.make_async_copy(closed_loop_h.at[part], am.at[part], a_sem.at[n])
        for n, part in enumerate((first_half, last_half))
    ]
    pairs = [
        (states_h, states), (inputs_h, inputs), (input_map_h.at[top], bm.at[top]), (state_map_h.at[top], sm.at[top]),
        (multipliers_h, mult), (input_map_h.at[pl.ds(0, top)], bm.at[pl.ds(0, top)]),
        (state_map_h.at[pl.ds(0, 8)], sm.at[pl.ds(0, 8)]),
        (state_map_h.at[pl.ds(8, top - 8)], sm.at[pl.ds(8, top - 8)]), (state_weight_h, state_weight),
        (state_linear_h, state_linear), (input_linear_h, input_linear), (offset_h, offset), (upper_h, upper),
        (bound_h, bound), (active_h, active), (weight_h, iw), (value_h, vm), (feedback_h, fm), (gain_h, gm),
    ]
    in_copies = [pltpu.make_async_copy(s, d, in_sem.at[n if n < 14 else n - 14]) for n, (s, d) in enumerate(pairs)]
    for copy in in_copies[:5]:
        copy.start()
    for copy in a_copies:
        copy.start()

    barrier = pltpu.get_barrier_semaphore()
    for by in range(1, LINE):
        pl.semaphore_signal(barrier, inc=1, device_id=peer("tm_0", by), device_id_type=MESH)
    for i, j in offsets:
        pl.semaphore_signal(barrier, inc=1, device_id=in_plane(i, j), device_id_type=MESH)
    has_next(lambda: pl.semaphore_signal(barrier, inc=1, device_id=next_device, device_id_type=MESH))
    has_prev(lambda: pl.semaphore_signal(barrier, inc=1, device_id=prev_device, device_id_type=MESH))

    def predict(k):
        at = pl.ds(k, 1)
        predicted[at, :] = row_mv(sm[k], states[at, :]) + col_mv(inputs[at, :], bm[k])

    a_halves[0].wait()
    for i in range(count // 4):
        tree[i] = mm(am[2 * i + 1], am[2 * i])
    for copy in a_halves[1:] + in_copies[:5]:
        copy.wait()
    predict(top)
    edge[...] = jnp.broadcast_to(predicted[pl.ds(top, 1), :], (8, ns))
    for copy in in_copies[5:]:
        copy.start()
    for i in range(count // 4, count // 2):
        tree[i] = mm(am[2 * i + 1], am[2 * i])
    level = [tree[i] for i in range(count // 2)]
    while len(level) > 1:
        level = [mm(level[i + 1], level[i]) for i in range(0, len(level), 2)]
    phi[...] = level[0]
    gz[z] = level[0]

    ends = lax.div(place + last, last + 1) + lax.div(2 * last - place, last + 1)
    pl.semaphore_wait(barrier, (LINE - 1) + len(offsets) + ends)

    def remote(src, dst, send, recv, device):
        return pltpu.make_async_remote_copy(
            src_ref=src, dst_ref=dst, send_sem=send, recv_sem=recv, device_id=device, device_id_type=MESH
        )

    part = ns // 4
    high, low = pl.ds(0, 2 * part), pl.ds(2 * part, 2 * part)
    quarters = [pl.ds(n * part, part) for n in range(4)]

    def gather_maps(stage, axis, maps):
        at = spot[axis]
        right, left = peer(axis, 1), peer(axis, LINE - 1)
        before, behind = lax.rem(at + LINE - 1, LINE), lax.rem(at + 1, LINE)
        plan = [
            (at, quarters[0], right), (at, quarters[3], left), (at, quarters[1], right), (at, quarters[2], left),
            (at, low, right), (at, high, left),
            (before, quarters[0], right), (behind, quarters[3], left),
            (before, quarters[1], right), (behind, quarters[2], left),
        ]
        sems = (0, 0, 1, 1, 2, 2, 2, 2, 2, 2)
        copies = [
            remote(maps.at[s, rows], maps.at[s, rows], m_send.at[stage], m_recv.at[stage, n], dev)
            for n, (s, rows, dev) in zip(sems, plan)
        ]
        whole = remote(maps.at[pl.ds(0, 3)], maps.at[pl.ds(0, 2)], m_send.at[stage], m_recv.at[stage, 2], right)
        return copies, whole

    def relay(copies, maps, stage, turn):
        remote(maps.at[0, high], maps.at[0, high], m_send.at[stage], m_recv.at[stage, turn], peer("tm_0", 1)).wait_recv()
        run(copies[2 * turn + 6 : 2 * turn + 8])

    def gather_vectors(stage, axis, buf):
        at = spot[axis]
        copies = [
            remote(buf.at[at], buf.at[at], v_send.at[stage], v_recv.at[stage], peer(axis, by)) for by in range(1, LINE)
        ]
        three = buf.at[pl.ds(0, LINE - 1)]
        return copies, remote(three, three, v_send.at[stage], v_recv.at[stage], peer(axis, 1))

    def run(copies):
        for copy in copies:
            copy.start()

    to_prev = remote(mult.at[pl.ds(0, 8)], from_next, e_send.at[0], e_recv.at[0], prev_device)
    to_next = remote(edge, from_prev, e_send.at[1], e_recv.at[1], next_device)
    z_maps, z_all = gather_maps(0, "tm_2", gz)
    has_prev(to_prev.start)
    has_next(to_next.start)
    half = count // 2

    @pl.when(core == 0)
    def _():
        run(z_maps[:6])

    qt[0] = identity_matrix(ns)
    qt[1] = jnp.transpose(am[0])
    qt[2] = jnp.transpose(tree[0])

    def prefix_step(i):
        prefix = qt[2 * i]
        qt[2 * i + 1] = mm(prefix, am[2 * i], 1, 1)
        qt[2 * i + 2] = mm(prefix, tree[i], 1, 1)

    pl.loop(1, half - 1)(prefix_step)
    qt[top] = mm(qt[top - 1], am[top - 1], 1, 1)

    @pl.when(core == 0)
    def _():
        relay(z_maps, gz, 0, 0)

    for copy in in_copies[5:8]:
        copy.wait()
    pl.loop(0, 10, unroll=5)(predict)

    @pl.when(core == 0)
    def _():
        relay(z_maps, gz, 0, 1)

    pl.loop(10, top, unroll=5)(predict)

    for copy in in_copies[8:16]:
        copy.wait()
    has_next(to_prev.wait_recv)

    @pl.when(place == last)
    def _():
        from_next[...] = jnp.zeros((8, ns), F32)

    following[pl.ds(0, top), :] = mult[pl.ds(1, top), :]
    following[pl.ds(top, 1), :] = from_next[pl.ds(0, 1), :]

    def gradients(k):
        at = pl.ds(k, 1)
        ahead = following[at, :]
        grad_state[at, :] = col_mv(ahead, sm[k])
        grad_input[at, :] = row_mv(bm[k], ahead)

    pl.loop(0, count, unroll=4)(gradients)
    grad_state[...] = state_weight[...] * states[...] + state_linear[...] + mult[...] - grad_state[...]
    weighted = lax.dot_general(
        inputs[...], iw[...], (((1,), (1,)), ((), ())), precision=PRECISE, preferred_element_type=F32
    )
    grad_input[...] = weighted + input_linear[...] - grad_input[...] + bound[...]

    def suffix_step(i):
        j = half - 1 - i
        suffix = rst[2 * j + 1]
        rst[2 * j] = mm(suffix, am[2 * j + 1])
        rst[2 * j - 1] = mm(suffix, tree[j])

    def suffixes():
        rst[top - 1] = am[top]
        rst[top - 2] = tree[half - 1]
        pl.loop(1, half - 1)(suffix_step)
        rst[0] = mm(rst[1], am[1])

    for copy in in_copies[16:]:
        copy.wait()
    has_prev(to_next.wait_recv)

    @pl.when(place == 0)
    def _():
        from_prev[...] = jnp.zeros((8, ns), F32)

    defect[pl.ds(1, top), :] = states[pl.ds(1, top), :] - predicted[pl.ds(0, top), :] - offset[pl.ds(1, top), :]
    entered = from_prev[pl.ds(0, 1), :]
    defect[pl.ds(0, 1), :] = states[pl.ds(0, 1), :] - entered - offset[pl.ds(0, 1), :]

    def source(k):
        at = pl.ds(k, 1)
        sources[at, :] = row_mv(vm[k], defect[at, :]) + grad_state[at, :] + col_mv(grad_input[at, :], fm[k])
        weighted_map[k] = mm(gm[k], bm[k])

    pl.loop(0, count, unroll=4)(source)

    @pl.when(core == 1)
    def _():
        run(z_maps[:6])
        suffixes()

    @pl.when(core == 1)
    def _():
        relay(z_maps, gz, 0, 0)
        relay(z_maps, gz, 0, 1)


    def gather_source(k, acc):
        return acc + fold(qt[k] * sources[pl.ds(k, 1), :])

    acc = lax.fori_loop(1, count, gather_source, jnp.zeros((ns, HALF), F32), unroll=3)
    local_costate = across(acc) + sources[pl.ds(0, 1), :]
    cvec[pl.ds(0, 1), :] = local_costate

    slack = bound[...] * (upper[...] - inputs[...])
    lane = lax.broadcasted_iota(jnp.int32, (1, ns), 1)
    squares = lambda t: jnp.sum(t * t)
    sums = [
        squares(defect[...]), squares(grad_state[...]) + squares(grad_input[...]), squares(slack),
        squares(offset[...]), squares(state_linear[...]) + squares(input_linear[...]), squares(bound[...]),
    ]
    stats = jnp.zeros((1, ns), F32)
    for n, s in enumerate(sums):
        stats = jnp.where(lane == n, s, stats)

    cz[z, pl.ds(0, 1), :] = local_costate
    cz[z, pl.ds(1, 1), :] = stats
    cz[z, pl.ds(2, 6), :] = jnp.zeros((6, ns), F32)
    c_line, c_all = gather_vectors(0, "tm_2", cz)
    run(c_line)

    def reach(k):
        both = jnp.concatenate([bm[k], weighted_map[k]], axis=0)
        w = mm(both, rst[k], 1, 1)
        rows = pl.ds(pl.multiple_of(k * nu, nu), nu)
        wst[rows, :] = w[:nu]
        gwst[rows, :] = w[nu:]

    def reach_all():
        pl.loop(0, top, unroll=5)(reach)
        wst[pl.ds(top * nu, nu), :] = bm[top]
        gwst[pl.ds(top * nu, nu), :] = weighted_map[top]

    pl.when(core == 1)(reach_all)

    z_all.wait_recv()
    gx[x] = line_products(gz, sz, pz)
    x_maps, x_all = gather_maps(1, "tm_1", gx)

    def line_backward(buf, maps, store):
        v = buf[LINE - 1, pl.ds(0, 1), :]
        store[LINE - 1] = jnp.zeros((8, ns), F32)
        for p in reversed(range(LINE - 1)):
            store[p] = jnp.broadcast_to(v, (8, ns))
            v = col_mv(v, maps[p]) + buf[p, pl.ds(0, 1), :]
        total = jnp.sum(buf[:, 1:2, :], axis=0)
        return v, total

    run(x_maps[:6])

    pl.when(core == 0)(suffixes)

    c_all.wait_recv()
    group_costate, totals = line_backward(cz, gz, vloc_z)
    cx[x, pl.ds(0, 1), :] = group_costate
    cx[x, pl.ds(1, 1), :] = totals
    cx[x, pl.ds(2, 6), :] = jnp.zeros((6, ns), F32)
    cx_line, cx_all = gather_vectors(1, "tm_1", cx)
    run(cx_line)

    pl.when(core == 0)(lambda: relay(x_maps, gx, 1, 0))

    def backward(i, v):
        k = top - i
        after[pl.ds(k, 1), :] = v
        return col_mv(v, am[k]) + sources[pl.ds(k, 1), :]

    v = lax.fori_loop(0, half // 2, backward, jnp.zeros((1, ns), F32))
    pl.when(core == 0)(lambda: relay(x_maps, gx, 1, 1))
    lax.fori_loop(half // 2, count, backward, v)

    @pl.when(core == 1)
    def _():
        relay(x_maps, gx, 1, 0)
        relay(x_maps, gx, 1, 1)

    def respond(k):
        at = pl.ds(k, 1)
        pull = row_mv(bm[k], after[at, :])
        pulled[at, :] = pull
        step = -row_mv(gm[k], grad_input[at, :] + pull)
        gain[at, :] = step
        pushes[at, :] = col_mv(step, bm[k])

    def gather_push(k, acc):
        return acc + fold(rst[k] * (pushes[pl.ds(k, 1), :] - defect[pl.ds(k + 1, 1), :]))

    def local_state():
        pl.loop(0, count, unroll=8)(respond)
        acc = lax.fori_loop(0, top, gather_push, -fold(phi[...] * defect[pl.ds(0, 1), :]), unroll=3)
        fvec[...] = jnp.broadcast_to(across(acc) + pushes[pl.ds(top, 1), :], (8, ns))

    local_state()

    def gather_reach():
        pl.when(core == 0)(reach_all)
        mmat[...] = mm(wst[...], gwst[...], 0, 0)

    line_rest(gz, sz, pz)
    cx_all.wait_recv()

    x_all.wait_recv()
    plane_costate, totals = line_backward(cx, gx, vloc_x)

    down = remote(dy, vy, e_send.at[2], e_recv.at[2], peer("tm_0", LINE - 1))

    @pl.when(y == LINE - 1)
    def _():
        dy[...] = jnp.broadcast_to(plane_costate, (8, ns))
        down.start()

    omega[...] = line_products(gx, sx, px)

    halves = (high, low)
    second = [remote(omega.at[r], om1.at[r], y_send.at[0], y_recv.at[n], peer("tm_0", 1)) for n, r in enumerate(halves)]
    third = remote(omega, om2, y_send.at[0], y_recv.at[2], peer("tm_0", 1))
    passed = [remote(om1.at[r], om1.at[r], y_send.at[1], y_recv.at[n], peer("tm_0", 1)) for n, r in enumerate(halves)]

    def pass_on(n):
        second[n].wait_recv()
        passed[n].start()

    @pl.when(y == 1)
    def _():
        run(second)

    @pl.when(y == 2)
    def _():
        third.start()

    sy[y] = jnp.broadcast_to(totals, (8, ns))
    s_line, s_all = gather_vectors(2, "tm_0", sy)
    run(s_line)
    line_rest(gx, sx, px)
    tback[...] = mm(sx[x], sz[z])
    t_zero = col_mv(vloc_x[x, pl.ds(0, 1), :], sz[z]) + vloc_z[z, pl.ds(0, 1), :]

    def combine():
        inward = mm(tback[...], mmat[...])
        answer[...] = mm(inward, tback[...], 1, 1)
        constant = row_mv(tback[...], fvec[pl.ds(0, 1), :]) - row_mv(inward, t_zero)
        avec[...] = jnp.broadcast_to(constant, (8, ns))

    @pl.when(y == 0)
    def _():
        gather_reach()
        combine()

    pl.when(y == 1)(gather_reach)

    @pl.when(y == LINE - 1)
    def _():
        vy[...] = jnp.zeros((8, ns), F32)

    @pl.when(y < LINE - 1)
    def _():
        down.wait_recv()

    plane_in = vy[pl.ds(0, 1), :]

    @pl.when((y == 1) | (y == 2))
    def _():
        dy[...] = jnp.broadcast_to(col_mv(plane_in, omega[...]) + plane_costate, (8, ns))
        down.start()

    @pl.when(y > 1)
    def _():
        gather_reach()

    pl.when(y > 0)(combine)

    here = x * LINE + z
    plane_sum[here, pl.ds(0, 1), :] = avec[pl.ds(0, 1), :] - row_mv(answer[...], plane_in)

    def to_plane(buf, rows, n):
        return [
            remote(buf.at[here, rows], buf.at[here, rows], p_send.at[n], p_recv.at[n], in_plane(i, j)) for i, j in offsets
        ]

    sum_rows, own_rows = pl.ds(0, 1), pl.ds(0, 2)
    run(to_plane(plane_sum, sum_rows, 0))
    v = col_mv(plane_in, tback[...]) + t_zero
    f_own = fvec[pl.ds(0, 1), :] - row_mv(mmat[...], v)
    plane_own[here, pl.ds(0, 1), :] = row_mv(sz[z], f_own)
    plane_own[here, pl.ds(1, 1), :] = f_own
    run(to_plane(plane_own, own_rows, 1))
    others = pl.ds(0, LINE * LINE - 1)
    sum_line = remote(plane_sum.at[others, sum_rows], plane_sum.at[others, sum_rows], p_send.at[0], p_recv.at[0], peer("tm_1", 1))
    own_line = remote(plane_own.at[others, own_rows], plane_own.at[others, own_rows], p_send.at[1], p_recv.at[1], peer("tm_1", 1))

    pl.when(y == 2)(lambda: pass_on(0))

    vc = as_column(v)

    def lift(k):
        at = pl.ds(k, 1)
        after[at, :] = after[at, :] + col_apply(vc, rst[k])

    pl.loop(0, top, unroll=5)(lift)
    after[pl.ds(top, 1), :] = v
    before_first = col_apply(vc, phi[...]) + cvec[pl.ds(0, 1), :]

    pl.loop(0, count, unroll=8)(respond)

    pl.when(y == 2)(lambda: pass_on(1))

    def forward(k, carried):
        correction = carried - defect[pl.ds(k, 1), :]
        state_step[pl.ds(k, 1), :] = correction
        return row_mv(am[k], correction) + pushes[pl.ds(k, 1), :]

    def local_steps():
        lax.fori_loop(0, count, forward, jnp.zeros((1, ns), F32))

    local_steps()

    sum_line.wait_recv()
    plane_state = jnp.sum(plane_sum[:, 0:1, :], axis=0)
    fy[y] = jnp.broadcast_to(plane_state, (8, ns))
    ahead = [
        remote(fy.at[y], fy.at[y], f_send.at[by - 1], f_recv.at[by - 1], peer("tm_0", by)) for by in range(1, LINE)
    ]
    for by in range(1, LINE):
        @pl.when(y + by < LINE)
        def _(by=by):
            ahead[by - 1].start()

    own_line.wait_recv()
    tforw[...] = mm(pz[z], px[x])

    def line_state(vector, maps, at):
        entering = jnp.zeros((1, ns), F32)
        found = entering
        for p in range(LINE - 1):
            entering = row_mv(maps[p], entering) + vector(p) if p else vector(p)
            found = jnp.where(at == p + 1, entering, found)
        return found

    in_line = line_state(lambda p: plane_own[x * LINE + p, pl.ds(1, 1), :], gz, z)
    groups = [jnp.sum(plane_own[LINE * p : LINE * p + LINE, 0:1, :], axis=0) for p in range(LINE)]
    in_group = line_state(lambda p: groups[p], gx, x)
    x_zero = row_mv(pz[z], in_group) + in_line

    s_all.wait_recv()
    totals = jnp.sum(sy[:, 0:1, :], axis=0)
    horizon = count * LINE**3
    pick = lambda n: jnp.sum(jnp.where(lane == n, totals, 0.0), axis=1, keepdims=True)
    primal = pick(0) / (pick(3) + floor_share * horizon * ns)
    dual = pick(1) / (pick(4) + floor_share * horizon * (ns + nu))
    complement = pick(2) / (pick(5) + floor_share * horizon * nu)
    lanes = lax.broadcasted_iota(jnp.int32, (8, ns), 1)
    values = jnp.where(lanes == 0, primal, jnp.where(lanes == 1, dual, complement))
    packed[pl.ds(3 * count, 8), :] = jnp.sqrt(values)

    at_plane = lambda p: fy[p, pl.ds(0, 1), :]

    def set_base(vector):
        avec[...] = jnp.broadcast_to(vector, (8, ns))

    @pl.when(y <= 1)
    def _():
        set_base(x_zero)

    @pl.when(y == 2)
    def _():
        through = tforw[...]
        tforw[...] = mm(through, om1[...])
        ahead[0].wait_recv()
        set_base(row_mv(through, at_plane(1)) + x_zero)

    @pl.when(y == LINE - 1)
    def _():
        through = tforw[...]
        third.wait_recv()
        for copy in passed:
            copy.wait_recv()
        tforw[...] = mm(mm(through, om2[...]), om1[...])
        ahead[0].wait_recv()
        ahead[1].wait_recv()
        set_base(row_mv(through, row_mv(om2[...], at_plane(1)) + at_plane(2)) + x_zero)

    @pl.when(y == 0)
    def _():
        entry[...] = avec[...]

    for by in range(1, LINE):
        @pl.when(y == by)
        def _(by=by):
            ahead[by - 1].wait_recv()
            entry[...] = jnp.broadcast_to(row_mv(tforw[...], at_plane(0)), (8, ns)) + avec[...]

    x_in = entry[pl.ds(0, 1), :]
    xc = as_column(x_in)

    def close(k):
        at = pl.ds(k, 1)
        now = state_step[at, :] + col_apply(xc, qt[k])
        packed[at, :] = now
        sources[at, :] = row_mv(vm[k], now - defect[at, :])
        input_linear[at, :] = row_mv(fm[k], now)

    pl.loop(0, count, unroll=8)(close)
    packed[pl.ds(count + 1, top), :] = sources[pl.ds(1, top), :] + after[pl.ds(0, top), :]
    packed[pl.ds(count, 1), :] = sources[pl.ds(0, 1), :] + before_first
    chosen = active[...].astype(F32)
    step = (1.0 - chosen) * (input_linear[...] + gain[...]) + chosen * (upper[...] - inputs[...])
    packed[pl.ds(2 * count, count), pl.ds(0, nu)] = step
    weighted = lax.dot_general(
        step, iw[...], (((1,), (1,)), ((), ())), precision=PRECISE, preferred_element_type=F32
    )
    packed[pl.ds(2 * count, count), pl.ds(HALF, nu)] = chosen * (grad_input[...] + weighted + pulled[...])

    has_prev(to_prev.wait_send)
    has_next(to_next.wait_send)
    for copy in [z_all, x_all, c_all, cx_all, s_all, sum_line, own_line]:
        copy.wait_send()

    for by in range(1, LINE):
        @pl.when(y + by < LINE)
        def _(by=by):
            ahead[by - 1].wait_send()

    @pl.when((y == 1) | (y == 2))
    def _():
        third.wait_send()

    @pl.when(y == 2)
    def _():
        remote(om1, om1, y_send.at[1], y_recv.at[0], peer("tm_0", 1)).wait_send()

    @pl.when(y > 0)
    def _():
        down.wait_send()


def unpack(packed, state_step, input_step, multiplier_step, bound_step, norms):
    count, nu = input_step.shape
    state_step[...] = packed[pl.ds(0, count), :]
    multiplier_step[...] = packed[pl.ds(count, count), :]
    input_step[...] = packed[pl.ds(2 * count, count), pl.ds(0, nu)]
    bound_step[...] = packed[pl.ds(2 * count, count), pl.ds(HALF, nu)]
    norms[...] = packed[pl.ds(3 * count, 1), pl.ds(0, HALF)][0, :3]


def local(*args):
    states, inputs = args[12], args[13]
    count, ns = states.shape
    nu = inputs.shape[1]
    v = lambda *shape: pltpu.VMEM(shape, F32)
    dma = lambda *shape: pltpu.SemaphoreType.DMA(shape)
    square = v(ns, ns)
    line = v(LINE, ns, ns)
    rows = v(LINE, 8, ns)
    row = v(8, ns)
    wide, narrow = v(count, ns), v(count, nu)
    scratch = [
        v(count, ns, ns), v(count, nu, ns), v(count, ns, ns), v(count, nu, ns), v(count, ns, ns),
        v(count, nu, nu), v(nu, nu), wide, wide, narrow, wide, narrow,
        wide, narrow, wide, narrow, pltpu.VMEM((count, nu), jnp.int32),
        v(count, ns, ns), v(count, ns, ns), v(count // 2, ns, ns), square, v(count, nu, ns), square, v(count * nu, ns), v(count * nu, ns),
        line, line, line, line, line, line, square, square, square, square, square,
        wide, wide, wide, wide, narrow, wide, wide, narrow, narrow, wide, wide,
        row, row, row, rows, rows, v(LINE * LINE, 8, ns), v(LINE * LINE, 8, ns), rows, row, row, row, row, row, square, rows,
        rows, rows, row,
        dma(14), dma(2), dma(2), dma(2, 3), dma(3), dma(3), dma(3), dma(3),
        dma(2), dma(2), dma(2), dma(3), dma(LINE - 1), dma(LINE - 1),
    ]
    vmem = pl.BlockSpec(memory_space=pltpu.VMEM)
    packed = pl.pallas_call(
        kernel,
        out_shape=pltpu.VMEM((3 * count + 8, ns), F32),
        in_specs=[pl.BlockSpec(memory_space=pl.ANY)] * len(args),
        out_specs=vmem,
        scratch_shapes=scratch,
        compiler_params=pltpu.CompilerParams(
            collective_id=0, has_side_effects=True, vmem_limit_bytes=56 * 1024 * 1024
        ),
        name="riccati",
    )(*args)
    return pl.pallas_call(
        unpack,
        out_shape=[
            jax.ShapeDtypeStruct((count, ns), F32),
            jax.ShapeDtypeStruct((count, nu), F32),
            jax.ShapeDtypeStruct((count, ns), F32),
            jax.ShapeDtypeStruct((count, nu), F32),
            jax.ShapeDtypeStruct((3,), F32),
        ],
        in_specs=[vmem],
        out_specs=[vmem] * 5,
        name="unpack",
    )(pltpu.with_memory_space_constraint(packed, pltpu.VMEM))


def solution(mesh):
    lines = Mesh(
        mesh.devices.reshape(LINE, LINE, LINE, mesh.shape["batch"]), ("tm_0", "tm_1", "tm_2", "batch")
    )
    cube, flat = P(BATCH_TM, None, None), P(BATCH_TM, None)
    return jax.shard_map(
        local,
        mesh=lines,
        in_specs=(cube,) * 6 + (P("batch", None),) + (flat,) * 10,
        out_specs=(flat, flat, flat, flat, P("batch")),
        check_vma=False,
    )
```
